256 devices in a mesh: groups: 2 (over z), ep: 128 (over y, x, core).
Axes of the slice: x: 8, y: 8, z: 2, core: 2. Of those that a mesh axis runs over, the one named last changes fastest.
The devices are a block of a 8x8x16 slice.
Arguments:
- tokens: bfloat16 [2048, 2880], P(('groups', 'ep')), parts along dimension 0, may hold values from -6 to 6
- norm_gain: float32 [2880], replicated, may hold values from 0.1 to 1.9
- expert_ids: int32 [2048, 4], P(('groups', 'ep')), parts along dimension 0, may hold values from 0 to 63, all different within a row; in each aligned block of 8 rows (0 to 7, 8 to 15, ...) at most 1 rows name the same one
- gate_codes: int32 [2048, 4], P(('groups', 'ep')), parts along dimension 0, may hold values from 1 to 65535
- w_gate: bfloat16 [128, 2880, 720], P('ep'), may hold values from -0.109375 to 0.109375
- w_up: bfloat16 [128, 2880, 720], P('ep'), may hold values from -0.109375 to 0.109375
- w_down: bfloat16 [128, 720, 2880], P('ep'), may hold values from -0.15625 to 0.15625
Outputs:
- updated: bfloat16 [2048, 2880], P(('groups', 'ep')), parts along dimension 0
The draws below stay inside these ranges and needn't reach their ends.
There are 2 independent parts, one for each index of `groups`. The reference program is written for one: setup_inputs(seed, part) draws one part's arguments, and reference() takes and returns one part's arrays. A program takes and returns all parts, laid end to end along the dimension named above; an argument that names none is the same for every part. Nothing has to cross between parts.
Inputs may be any that keep to these rules, and one draw needn't show every extreme that they name: `expert_ids`: each token names 4 different experts. Among the tokens of one device (aligned blocks of 8 rows) no expert is named more than once, and in every draw some expert is named exactly once by some device's tokens.
All inputs are finite; a program needn't handle non-finite values.
Results may differ from the reference program's by a relative error of at most 0.0049.
Values may be sent and summed in bfloat16 or wider, within the bound.
A program may use at most 64 MiB of HBM per device.

```python
import math
import jax
import jax.numpy as jnp
import numpy as np
from jax import lax

D = 2880
FF = 1440
TOP = 4
HALVES = 2
TOK_DEV = 8
EXPERTS = 64
SHARD_FF = 720
CAP = 1
TOKENS = 1024
N_EP = 128


def plant(entries, stream_key, smallest, high):
    place = [jax.random.randint(jax.random.fold_in(stream_key, axis), (), 0, length) for axis, length in enumerate(entries.shape)]
    main_axis = entries.shape.index(max(entries.shape))
    beside = place[:main_axis] + [(place[main_axis] + 1) % entries.shape[main_axis]] + place[main_axis + 1:]
    return entries.at[tuple(place)].set(smallest).at[tuple(beside)].set(high)


def block_levels(key, shape, split, low, high):
    def one(position, shards_of):
        steps = jax.random.uniform(jax.random.fold_in(jax.random.fold_in(key, 6), position), (shards_of,), jnp.float32, low / len(split), high / len(split))
        return jnp.repeat(jnp.exp(steps), shape[position] // shards_of).reshape((-1,) + (1,) * (len(shape) - position - 1))

    factor_of = one(*split[0])
    for cut in split[1:]:
        factor_of = factor_of * one(*cut)
    return factor_of


def assign_block(stream_key, own, number, rows, count, top, bound, skew):
    sequence = jax.random.permutation(stream_key, count)
    packed, usual = load_shares(count, rows * top, bound, skew, True), load_shares(count, rows * top, bound, skew, False)
    places = jnp.arange(count)

    def named(sizes, turn):
        used = int((sizes > 0).sum())
        fixed = max(1, used // 4)
        moved = fixed + (places - fixed + turn * (used - fixed)) % max(1, count - fixed)
        return jnp.zeros((count,), jnp.int32).at[sequence[jnp.where(places < fixed, places, moved)]].set(jnp.asarray(sizes, jnp.int32))

    sizes = jnp.where(number % 4 == 0, named(packed, number // 4), named(usual, number - number // 4 - 1))
    mixed = jax.random.permutation(jax.random.fold_in(own, 3), count)
    source_of, taker = mixed[0:count // 2 * 2:2], mixed[1:count // 2 * 2:2]
    slack = jnp.minimum(sizes[source_of] - 1, bound - sizes[taker]) // 2
    slack = jnp.where((source_of == sequence[0]) | (taker == sequence[0]) | (sizes[taker] == 0), 0, jnp.maximum(slack, 0))
    moved = jax.random.randint(jax.random.fold_in(own, 4), (count // 2,), 0, 1 << 20) % (slack + 1)
    sizes = sizes.at[source_of].add(-moved).at[taker].add(moved)
    labels = jnp.searchsorted(jnp.cumsum(sizes), jnp.arange(rows * top), side="right").astype(jnp.int32)
    table = labels.reshape(top, rows).T
    table = table[jax.random.permutation(jax.random.fold_in(own, 1), rows)]
    turn = jax.random.randint(jax.random.fold_in(own, 2), (rows, 1), 0, top)
    return jnp.take_along_axis(table, (jnp.arange(top)[None, :] + turn) % top, axis=1)


def load_shares(number_of, total, most, slope, full):
    weights = [(1 << 20) // math.isqrt(rank ** slope) + 1 for rank in range(1, number_of + 1)]
    largest = most if full else min(most, max(-(-total // number_of), total * weights[0] // sum(weights)))
    least = 1 if total - largest >= number_of - 1 else 0
    holding, rest = [largest] + [least] * (number_of - 1), total - largest - least * (number_of - 1)
    while rest > 0:
        movable = [i for i in range(1, number_of) if holding[i] < largest] or [i for i in range(1, number_of) if holding[i] < most]
        whole, left = sum([weights[i] for i in movable]), rest
        for i in movable:
            extra = min(most - holding[i], max(1, left * weights[i] // whole), rest)
            holding[i] = holding[i] + extra
            rest = rest - extra
    return np.array(holding)


def noise(key, shape, scale, bound, split=(), kind=jnp.bfloat16):
    drawn = jax.random.normal(key, shape, jnp.float32) * scale
    if len(split) > 0:
        drawn = block_levels(key, shape, split, -0.22, 0.18) * drawn
    return jnp.clip(drawn, min=-bound, max=bound).astype(kind)


def setup_inputs(seed: int = 0, part: int = 0) -> dict:
    arg_keys = jax.random.split(jax.random.key(seed), 8)
    part_splits = jax.random.split(jax.random.fold_in(arg_keys[7], part), 8)
    tokens = noise(part_splits[0], (TOKENS, D), 1.0, 6.0, ((0, 128),))
    norm_gain = jnp.clip(1.0 + 0.18 * jax.random.normal(arg_keys[1], (D,), jnp.float32), 0.1, 1.9)
    expert_ids_keys = jax.random.split(jax.random.fold_in(part_splits[2], 1), TOKENS // TOK_DEV)
    expert_ids_turns = jax.random.permutation(jax.random.fold_in(part_splits[2], 3), TOKENS // TOK_DEV)
    expert_ids = jax.vmap(lambda own, number: assign_block(jax.random.fold_in(part_splits[2], 2), own, number, TOK_DEV, EXPERTS, TOP, CAP, 2))(expert_ids_keys, expert_ids_turns).reshape((TOKENS, TOP))
    gate_codes = plant(jax.random.randint(part_splits[3], (TOKENS, TOP), 1, 65536), jax.random.fold_in(part_splits[3], 1), 1, 65535).astype(jnp.int32)
    w_gate = noise(arg_keys[4], (EXPERTS * HALVES, D, SHARD_FF), D ** -0.5, 0.109375, ((0, 128),))
    w_up = noise(arg_keys[5], (EXPERTS * HALVES, D, SHARD_FF), D ** -0.5, 0.109375, ((0, 128),))
    w_down = noise(arg_keys[6], (EXPERTS * HALVES, SHARD_FF, D), FF ** -0.5, 0.15625, ((0, 128),))
    return dict(tokens=tokens, norm_gain=norm_gain, expert_ids=expert_ids, gate_codes=gate_codes, w_gate=w_gate, w_up=w_up, w_down=w_down)


epsilon = 1e-05

def reference(tokens, norm_gain, expert_ids, gate_codes, w_gate, w_up, w_down):
    values = tokens.astype(jnp.float32)
    normed = (values * lax.rsqrt(lax.optimization_barrier(jnp.mean(values * values, axis=1, keepdims=True)) + epsilon) * norm_gain).astype(jnp.bfloat16)
    code_values = gate_codes.astype(jnp.float32)
    weights = code_values / lax.optimization_barrier(jnp.sum(code_values, axis=1, keepdims=True))
    pair_total = TOKENS * TOP
    room = N_EP * CAP
    flat_ids = expert_ids.reshape(-1).astype(jnp.int32)
    gates_all = w_gate.reshape(EXPERTS, HALVES, D, SHARD_FF)
    ups_all = w_up.reshape(EXPERTS, HALVES, D, SHARD_FF)
    downs_all = w_down.reshape(EXPERTS, HALVES, SHARD_FF, D)

    def one_expert(expert, per_pair):
        indices = jnp.nonzero(flat_ids == expert, size=room, fill_value=pair_total)[0].astype(jnp.int32)
        token_rows = normed[jnp.minimum(indices, pair_total - 1) // TOP].astype(jnp.float32)
        gate_mat = lax.dynamic_index_in_dim(gates_all, expert, 0, keepdims=False)
        gate_mat = jnp.transpose(gate_mat, (1, 0, 2)).reshape(D, FF).astype(jnp.float32)
        up_mat = lax.dynamic_index_in_dim(ups_all, expert, 0, keepdims=False)
        up_mat = jnp.transpose(up_mat, (1, 0, 2)).reshape(D, FF).astype(jnp.float32)
        down_mat = lax.dynamic_index_in_dim(downs_all, expert, 0, keepdims=False).astype(jnp.float32)
        gate_out = jnp.dot(token_rows, gate_mat, precision=lax.Precision.HIGHEST, preferred_element_type=jnp.float32)
        upward = jnp.dot(token_rows, up_mat, precision=lax.Precision.HIGHEST, preferred_element_type=jnp.float32)
        hidden = (jax.nn.silu(gate_out) * upward).astype(jnp.bfloat16).astype(jnp.float32)
        share_low = jnp.dot(hidden[:, :SHARD_FF], down_mat[0], precision=lax.Precision.HIGHEST, preferred_element_type=jnp.float32).astype(jnp.bfloat16)
        share_high = jnp.dot(hidden[:, SHARD_FF:], down_mat[1], precision=lax.Precision.HIGHEST, preferred_element_type=jnp.float32).astype(jnp.bfloat16)
        output = (share_low.astype(jnp.float32) + share_high.astype(jnp.float32)).astype(jnp.bfloat16)
        return per_pair.at[indices].set(output, mode='drop')
    per_pair = lax.fori_loop(0, EXPERTS, one_expert, jnp.zeros((pair_total, D), jnp.bfloat16))
    mixture = lax.optimization_barrier(jnp.sum(per_pair.reshape(TOKENS, TOP, D).astype(jnp.float32) * weights[:, :, None], axis=1))
    return (values + mixture).astype(jnp.bfloat16)
```

```python
import functools
import math

import jax
import jax.numpy as jnp
from jax import lax
from jax.experimental import pallas as pl
from jax.experimental.pallas import tpu as pltpu
from jax.sharding import PartitionSpec as P

epsilon = 1e-05
MESH = pl.DeviceIdType.MESH
F32 = jnp.float32
BF16 = jnp.bfloat16


def order_of(side):
    return sorted(range(1, side), key=lambda d: -min(d, side - d))


def kernel(
    side,
    tokens_hbm, gain_hbm, ids_hbm, codes_hbm, gate_hbm, up_hbm, down_hbm,
    out_ref,
    tokens_v, gain_v, ids_v, codes_v, gate_v, up_v, down_v,
    picked, relayed, turned, mine, other, given, taken, summed, back, unturned, results,
    load_sem, weight_sem,
    send1, recv1, send2, recv2, send_x, recv_x, send_y, recv_y, send3, recv3, send4, recv4,
):
    me = lax.axis_index("ep")
    core = lax.rem(me, 2)
    chip = me // 2
    row, column = chip // side, lax.rem(chip, side)
    p = jnp.where(core == 0, column, row)
    q = jnp.where(core == 0, row, column)
    slots = side * side

    def device(p_of, q_of):
        y = jnp.where(core == 0, q_of, p_of)
        x = jnp.where(core == 0, p_of, q_of)
        return {"ep": (y * side + x) * 2 + core}

    partner = {"ep": me + 1 - 2 * core}
    far_first = order_of(side)

    small = [
        pltpu.make_async_copy(src, dst, load_sem.at[i])
        for i, (src, dst) in enumerate(
            [(tokens_hbm, tokens_v), (gain_hbm, gain_v), (ids_hbm, ids_v), (codes_hbm, codes_v)]
        )
    ]
    for copy in small:
        copy.start()
    weights = [
        pltpu.make_async_copy(src.at[0], dst, weight_sem.at[i])
        for i, (src, dst) in enumerate([(gate_hbm, gate_v), (up_hbm, up_v), (down_hbm, down_v)])
    ]

    barrier = pltpu.get_barrier_semaphore()
    for d in far_first:
        pl.semaphore_signal(barrier, inc=1, device_id=device(lax.rem(p + d, side), q), device_id_type=MESH)
        pl.semaphore_signal(barrier, inc=1, device_id=device(p, lax.rem(q + d, side)), device_id_type=MESH)
    pl.semaphore_signal(barrier, inc=1, device_id=partner, device_id_type=MESH)
    for copy in small:
        copy.wait()
    for copy in weights:
        copy.start()

    values = tokens_v[...].astype(F32)
    normed = values * lax.rsqrt(jnp.mean(values * values, axis=1, keepdims=True) + epsilon) * gain_v[...]
    normed = normed.astype(BF16)
    lane = lax.broadcasted_iota(jnp.int32, (tokens_v.shape[0], slots), 1)
    minor, major = lax.rem(lane, side), lane // side
    expert = jnp.where(core == 0, minor * side + major, lane)
    codes = codes_v[...].astype(F32)
    share = codes / jnp.sum(codes, axis=1, keepdims=True)
    chosen = jnp.zeros(lane.shape, F32)
    mix = jnp.zeros(lane.shape, F32)
    for k in range(ids_v.shape[1]):
        hit = ids_v[:, k : k + 1] == expert
        chosen = jnp.where(hit, 1.0, chosen)
        mix = jnp.where(hit, share[:, k : k + 1], mix)
    rows = lax.dot_general(
        chosen.astype(BF16), normed, (((0,), (0,)), ((), ())), preferred_element_type=F32
    )
    picked[...] = rows.astype(BF16).reshape(picked.shape)

    a = lax.broadcasted_iota(jnp.int32, (slots, slots), 0)
    b = lax.broadcasted_iota(jnp.int32, (slots, slots), 1)
    turn = jnp.where((a // side == lax.rem(b, side)) & (lax.rem(a, side) == b // side), 1.0, 0.0).astype(BF16)

    def turned_rows(ref):
        block = ref[...].reshape(slots, ref.shape[2])
        return jnp.dot(turn, block, preferred_element_type=F32).astype(BF16).reshape(ref.shape)

    pl.semaphore_wait(barrier, 2 * (side - 1) + 1)

    def scatter(src, dst, send, recv, place, device_of, own):
        copies = []
        for d in far_first:
            j = lax.rem(place + d, side)
            copy = pltpu.make_async_remote_copy(
                src_ref=src.at[j], dst_ref=dst.at[own], send_sem=send.at[j], recv_sem=recv.at[own],
                device_id=device_of(j), device_id_type=MESH,
            )
            copy.start()
            copies.append(copy)
        dst[own] = src[own]
        return copies

    def arrival(dst, send, recv, j):
        return pltpu.make_async_remote_copy(
            src_ref=dst.at[j], dst_ref=dst.at[j], send_sem=send.at[j], recv_sem=recv.at[j],
            device_id=partner, device_id_type=MESH,
        )

    near_first = far_first[::-1]
    along_p = lambda j: device(j, q)
    along_q = lambda j: device(p, j)
    sent = []
    sent += scatter(picked, relayed, send1, recv1, p, along_p, p)
    for d in near_first:
        arrival(relayed, send1, recv1, lax.rem(p + d, side)).wait_recv()
    turned[...] = turned_rows(relayed)
    sent += scatter(turned, mine, send2, recv2, q, along_q, q)

    for d in [0] + near_first:
        j = lax.rem(q + d, side)
        if d:
            arrival(mine, send2, recv2, j).wait_recv()
        copy = pltpu.make_async_remote_copy(
            src_ref=mine.at[j], dst_ref=other.at[j], send_sem=send_x.at[j], recv_sem=recv_x.at[j],
            device_id=partner, device_id_type=MESH,
        )
        copy.start()
        sent.append(copy)
    for copy in weights[:2]:
        copy.wait()
    for d in [0] + near_first:
        arrival(other, send_x, recv_x, lax.rem(q + d, side)).wait_recv()

    width = tokens_v.shape[1]
    arrived = jnp.concatenate([mine[...].reshape(slots, width), other[...].reshape(slots, width)], axis=0)
    gate_out = jnp.dot(arrived, gate_v[...], preferred_element_type=F32)
    upward = jnp.dot(arrived, up_v[...], preferred_element_type=F32)
    hidden = (gate_out / (1.0 + jnp.exp(-gate_out)) * upward).astype(BF16)
    weights[2].wait()
    partial = jnp.dot(hidden, down_v[...], preferred_element_type=F32).astype(BF16)
    given[...] = partial[slots:].reshape(given.shape)
    copy = pltpu.make_async_remote_copy(
        src_ref=given, dst_ref=taken, send_sem=send_y, recv_sem=recv_y, device_id=partner, device_id_type=MESH,
    )
    copy.start()
    copy.wait_recv()
    sent.append(copy)
    total = partial[:slots].astype(F32) + taken[...].reshape(slots, width).astype(F32)
    summed[...] = total.astype(BF16).reshape(summed.shape)

    sent += scatter(summed, back, send3, recv3, q, along_q, q)
    for d in near_first:
        arrival(back, send3, recv3, lax.rem(q + d, side)).wait_recv()
    unturned[...] = turned_rows(back)
    sent += scatter(unturned, results, send4, recv4, p, along_p, p)
    for d in near_first:
        arrival(results, send4, recv4, lax.rem(p + d, side)).wait_recv()
    block = results[...].reshape(slots, width)
    high = mix.astype(BF16)
    rest = mix - high.astype(F32)
    middle = rest.astype(BF16)
    low = (rest - middle.astype(F32)).astype(BF16)
    mixture = sum(jnp.dot(part, block, preferred_element_type=F32) for part in (low, middle, high))
    out_ref[...] = (tokens_v[...].astype(F32) + mixture).astype(BF16)
    for copy in sent:
        copy.wait_send()


def shards(tokens, norm_gain, expert_ids, gate_codes, w_gate, w_up, w_down):
    side = math.isqrt(lax.axis_size("ep") // 2)
    count, width = tokens.shape
    shard_ff = w_gate.shape[2]
    blocks = pltpu.VMEM((side, side, width), BF16)
    DMA = pltpu.SemaphoreType.DMA
    return pl.pallas_call(
        functools.partial(kernel, side),
        out_shape=jax.ShapeDtypeStruct((count, width), BF16),
        in_specs=[pl.BlockSpec(memory_space=pl.ANY)] * 7,
        out_specs=pl.BlockSpec(memory_space=pltpu.VMEM),
        scratch_shapes=[
            pltpu.VMEM((count, width), BF16),
            pltpu.VMEM((1, width), F32),
            pltpu.VMEM(expert_ids.shape, jnp.int32),
            pltpu.VMEM(gate_codes.shape, jnp.int32),
            pltpu.VMEM((width, shard_ff), BF16),
            pltpu.VMEM((width, shard_ff), BF16),
            pltpu.VMEM((shard_ff, width), BF16),
        ]
        + [blocks] * 11
        + [DMA((4,)), DMA((3,))]
        + [DMA((side,))] * 6
        + [DMA, DMA]
        + [DMA((side,))] * 4,
        compiler_params=pltpu.CompilerParams(
            collective_id=0, has_side_effects=True, vmem_limit_bytes=60 * 2**20
        ),
    )(tokens, norm_gain.reshape(1, width), expert_ids, gate_codes, w_gate, w_up, w_down)


def solution(mesh):
    return jax.shard_map(
        shards,
        mesh=mesh,
        in_specs=(
            P(("groups", "ep"), None),
            P(),
            P(("groups", "ep"), None),
            P(("groups", "ep"), None),
            P("ep", None, None),
            P("ep", None, None),
            P("ep", None, None),
        ),
        out_specs=P(("groups", "ep"), None),
        check_vma=False,
    )
```

```python
import functools
import math

import jax
import jax.numpy as jnp
from jax import lax
from jax.experimental import pallas as pl
from jax.experimental.pallas import tpu as pltpu
from jax.sharding import PartitionSpec as P

epsilon = 1e-05
MESH = pl.DeviceIdType.MESH
F32 = jnp.float32
BF16 = jnp.bfloat16
ROWS_BY_ROWS = (((1,), (1,)), ((), ()))
COLUMNS_BY_ROWS = (((0,), (0,)), ((), ()))


def order_of(side):
    return sorted(range(1, side), key=lambda d: -min(d, side - d))


def kernel(
    side,
    tokens_hbm, gain_hbm, ids_hbm, codes_hbm, gate_hbm, up_hbm, down_hbm,
    out_ref,
    tokens_v, gain_v, ids_v, codes_v, gate_v, up_v, down_v,
    picked, relayed, turned, mine, other, given, taken, summed, back, unturned, results,
    load_sem, weight_sem,
    send1, recv1, send2, recv2, send_x, recv_x, send_y, recv_y, send3, recv3, send4, recv4,
):
    me = lax.axis_index("ep")
    core = lax.rem(me, 2)
    chip = me // 2
    row, column = chip // side, lax.rem(chip, side)
    p = jnp.where(core == 0, column, row)
    q = jnp.where(core == 0, row, column)
    slots = side * side

    def device(p_of, q_of):
        y = jnp.where(core == 0, q_of, p_of)
        x = jnp.where(core == 0, p_of, q_of)
        return {"ep": (y * side + x) * 2 + core}

    partner = {"ep": me + 1 - 2 * core}
    far_first = order_of(side)

    small = [
        pltpu.make_async_copy(src, dst, load_sem.at[i])
        for i, (src, dst) in enumerate(
            [(tokens_hbm, tokens_v), (gain_hbm, gain_v), (ids_hbm, ids_v), (codes_hbm, codes_v)]
        )
    ]
    for copy in small:
        copy.start()
    weights = [
        pltpu.make_async_copy(src.at[0], dst, weight_sem.at[i])
        for i, (src, dst) in enumerate([(gate_hbm, gate_v), (up_hbm, up_v), (down_hbm, down_v)])
    ]

    barrier = pltpu.get_barrier_semaphore()
    for d in far_first:
        pl.semaphore_signal(barrier, inc=1, device_id=device(lax.rem(p + d, side), q), device_id_type=MESH)
        pl.semaphore_signal(barrier, inc=1, device_id=device(p, lax.rem(q + d, side)), device_id_type=MESH)
    pl.semaphore_signal(barrier, inc=1, device_id=partner, device_id_type=MESH)
    for copy in small:
        copy.wait()
    for copy in weights:
        copy.start()

    values = tokens_v[...].astype(F32)
    normed = values * lax.rsqrt(jnp.mean(values * values, axis=1, keepdims=True) + epsilon) * gain_v[...].reshape(1, -1)
    normed = normed.astype(BF16)
    slot = lax.broadcasted_iota(jnp.int32, (slots, tokens_v.shape[0]), 0)
    minor, major = lax.rem(slot, side), slot // side
    expert = jnp.where(core == 0, minor * side + major, slot)
    codes = codes_v[...].astype(F32)
    share = codes / jnp.sum(codes, axis=0, keepdims=True)
    chosen = jnp.zeros(slot.shape, F32)
    mix = jnp.zeros(slot.shape, F32)
    for k in range(ids_v.shape[0]):
        hit = ids_v[k : k + 1, :] == expert
        chosen = jnp.where(hit, 1.0, chosen)
        mix = jnp.where(hit, share[k : k + 1, :], mix)
    rows = jnp.dot(chosen.astype(BF16), normed, preferred_element_type=F32)
    picked[...] = rows.astype(BF16).reshape(picked.shape)

    a = lax.broadcasted_iota(jnp.int32, (slots, slots), 0)
    b = lax.broadcasted_iota(jnp.int32, (slots, slots), 1)
    turn = jnp.where((a // side == lax.rem(b, side)) & (lax.rem(a, side) == b // side), 1.0, 0.0).astype(BF16)

    def turned_rows(ref):
        block = ref[...].reshape(slots, ref.shape[2])
        return jnp.dot(turn, block, preferred_element_type=F32).astype(BF16).reshape(ref.shape)

    pl.semaphore_wait(barrier, 2 * (side - 1) + 1)

    def scatter(src, dst, send, recv, place, device_of, own):
        copies = []
        for d in far_first:
            j = lax.rem(place + d, side)
            copy = pltpu.make_async_remote_copy(
                src_ref=src.at[j], dst_ref=dst.at[own], send_sem=send.at[j], recv_sem=recv.at[own],
                device_id=device_of(j), device_id_type=MESH,
            )
            copy.start()
            copies.append(copy)
        dst[own] = src[own]
        return copies

    def arrival(dst, send, recv, j):
        return pltpu.make_async_remote_copy(
            src_ref=dst.at[j], dst_ref=dst.at[j], send_sem=send.at[j], recv_sem=recv.at[j],
            device_id=partner, device_id_type=MESH,
        )

    near_first = far_first[::-1]
    along_p = lambda j: device(j, q)
    along_q = lambda j: device(p, j)
    sent = []
    sent += scatter(picked, relayed, send1, recv1, p, along_p, p)
    for d in near_first:
        arrival(relayed, send1, recv1, lax.rem(p + d, side)).wait_recv()
    turned[...] = turned_rows(relayed)
    sent += scatter(turned, mine, send2, recv2, q, along_q, q)

    for d in [0] + near_first:
        j = lax.rem(q + d, side)
        if d:
            arrival(mine, send2, recv2, j).wait_recv()
        copy = pltpu.make_async_remote_copy(
            src_ref=mine.at[j], dst_ref=other.at[j], send_sem=send_x.at[j], recv_sem=recv_x.at[j],
            device_id=partner, device_id_type=MESH,
        )
        copy.start()
        sent.append(copy)
    for copy in weights[:2]:
        copy.wait()
    for d in [0] + near_first:
        arrival(other, send_x, recv_x, lax.rem(q + d, side)).wait_recv()

    width = tokens_v.shape[1]
    arrived = jnp.concatenate([mine[...].reshape(slots, width), other[...].reshape(slots, width)], axis=0)
    gate_out = lax.dot_general(gate_v[...], arrived, ROWS_BY_ROWS, preferred_element_type=F32)
    upward = lax.dot_general(up_v[...], arrived, ROWS_BY_ROWS, preferred_element_type=F32)
    hidden = (gate_out / (1.0 + jnp.exp(-gate_out)) * upward).astype(BF16)
    weights[2].wait()
    partial = lax.dot_general(hidden, down_v[...], COLUMNS_BY_ROWS, preferred_element_type=F32).astype(BF16)
    given[...] = partial[slots:].reshape(given.shape)
    copy = pltpu.make_async_remote_copy(
        src_ref=given, dst_ref=taken, send_sem=send_y, recv_sem=recv_y, device_id=partner, device_id_type=MESH,
    )
    copy.start()
    copy.wait_recv()
    sent.append(copy)
    total = partial[:slots].astype(F32) + taken[...].reshape(slots, width).astype(F32)
    summed[...] = total.astype(BF16).reshape(summed.shape)

    sent += scatter(summed, back, send3, recv3, q, along_q, q)
    for d in near_first:
        arrival(back, send3, recv3, lax.rem(q + d, side)).wait_recv()
    unturned[...] = turned_rows(back)
    sent += scatter(unturned, results, send4, recv4, p, along_p, p)
    for d in near_first:
        arrival(results, send4, recv4, lax.rem(p + d, side)).wait_recv()
    block = results[...].reshape(slots, width)
    high = mix.astype(BF16)
    rest = mix - high.astype(F32)
    middle = rest.astype(BF16)
    low = (rest - middle.astype(F32)).astype(BF16)
    mixture = sum(
        lax.dot_general(part, block, COLUMNS_BY_ROWS, preferred_element_type=F32) for part in (low, middle, high)
    )
    out_ref[...] = (tokens_v[...].astype(F32) + mixture).astype(BF16)
    for copy in sent:
        copy.wait_send()


def shards(tokens, norm_gain, expert_ids, gate_codes, w_gate, w_up, w_down):
    side = math.isqrt(lax.axis_size("ep") // 2)
    count, width = tokens.shape
    shard_ff = w_gate.shape[2]
    blocks = pltpu.VMEM((side, side, width), BF16)
    DMA = pltpu.SemaphoreType.DMA
    return pl.pallas_call(
        functools.partial(kernel, side),
        out_shape=jax.ShapeDtypeStruct((count, width), BF16),
        in_specs=[pl.BlockSpec(memory_space=pl.ANY)] * 7,
        out_specs=pl.BlockSpec(memory_space=pltpu.VMEM),
        scratch_shapes=[
            pltpu.VMEM((count, width), BF16),
            pltpu.VMEM((width,), F32),
            pltpu.VMEM(expert_ids.shape[::-1], jnp.int32),
            pltpu.VMEM(gate_codes.shape[::-1], jnp.int32),
            pltpu.VMEM((shard_ff, width), BF16),
            pltpu.VMEM((shard_ff, width), BF16),
            pltpu.VMEM((shard_ff, width), BF16),
        ]
        + [blocks] * 11
        + [DMA((4,)), DMA((3,))]
        + [DMA((side,))] * 6
        + [DMA, DMA]
        + [DMA((side,))] * 4,
        compiler_params=pltpu.CompilerParams(
            collective_id=0, has_side_effects=True, vmem_limit_bytes=60 * 2**20
        ),
    )(
        tokens, norm_gain, expert_ids.T, gate_codes.T,
        jnp.swapaxes(w_gate, 1, 2), jnp.swapaxes(w_up, 1, 2), w_down,
    )


def solution(mesh):
    return jax.shard_map(
        shards,
        mesh=mesh,
        in_specs=(
            P(("groups", "ep"), None),
            P(),
            P(("groups", "ep"), None),
            P(("groups", "ep"), None),
            P("ep", None, None),
            P("ep", None, None),
            P("ep", None, None),
        ),
        out_specs=P(("groups", "ep"), None),
        check_vma=False,
    )
```

```python
import functools
import math

import jax
import jax.numpy as jnp
from jax import lax
from jax.experimental import pallas as pl
from jax.experimental.pallas import tpu as pltpu
from jax.sharding import PartitionSpec as P

epsilon = 1e-05
MESH = pl.DeviceIdType.MESH
F32 = jnp.float32
BF16 = jnp.bfloat16
LANES = 128
ROWS_BY_ROWS = (((1,), (1,)), ((), ()))
COLUMNS_BY_ROWS = (((0,), (0,)), ((), ()))


def kernel(
    side, tiles,
    tokens_hbm, gain_hbm, ids_hbm, codes_hbm, gate_hbm, up_hbm, down_hbm,
    out_ref,
    tokens_v, gain_v, ids_v, ids_s, codes_s, gate_v, up_v, down_v,
    wide, picked, mine, other, arrived, given, taken, own_share, summed, results,
    load_sem, weight_sem,
    send1, recv1, send_x, recv_x, send_y, recv_y, send2, recv2,
):
    me = lax.axis_index("ep")
    core = lax.rem(me, 2)
    chip = me // 2
    row, column = chip // side, lax.rem(chip, side)
    chips = side * side
    count, width = tokens_v.shape
    top = ids_v.shape[0]
    padded = tiles * LANES
    used = pl.cdiv(width, LANES)
    partner = {"ep": me + 1 - 2 * core}

    near = lambda d: min(d, side - d)
    offsets = [(dy, dx) for dy in range(side) for dx in range(side) if dy or dx]
    offsets.sort(key=lambda o: -(near(o[0]) + near(o[1])))
    rows_at = [lax.rem(row + d, side) * side for d in range(side)]
    columns_at = [lax.rem(column + d, side) for d in range(side)]
    peers = [rows_at[dy] + columns_at[dx] for dy, dx in offsets]

    small = [
        pltpu.make_async_copy(src, dst, load_sem.at[i])
        for i, (src, dst) in enumerate(
            [(tokens_hbm, tokens_v), (gain_hbm, gain_v), (ids_hbm, ids_v), (ids_hbm, ids_s), (codes_hbm, codes_s)]
        )
    ]
    for copy in small:
        copy.start()
    weights = [
        pltpu.make_async_copy(src.at[0], dst, weight_sem.at[i])
        for i, (src, dst) in enumerate([(gate_hbm, gate_v), (up_hbm, up_v), (down_hbm, down_v)])
    ]

    barrier = pltpu.get_barrier_semaphore()
    for j in peers:
        pl.semaphore_signal(barrier, inc=1, device_id={"ep": 2 * j + core}, device_id_type=MESH)
    pl.semaphore_signal(barrier, inc=1, device_id=partner, device_id_type=MESH)
    for copy in small:
        copy.wait()
    for copy in weights:
        copy.start()

    values = tokens_v[...].astype(F32)
    normed = values * lax.rsqrt(jnp.mean(values * values, axis=1, keepdims=True) + epsilon) * gain_v[...].reshape(1, -1)
    normed = normed.astype(BF16)
    expert = lax.broadcasted_iota(jnp.int32, (chips, count), 0)
    chosen = jnp.zeros(expert.shape, F32)
    for k in range(top):
        chosen = jnp.where(ids_v[k : k + 1, :] == expert, 1.0, chosen)
    rows = jnp.dot(chosen.astype(BF16), normed, preferred_element_type=F32)

    def spread(value, base):
        n = value.shape[0]
        value = jnp.concatenate([value, jnp.zeros((n, padded - width), F32)], axis=1)
        for j in range(tiles):
            wide[pl.ds(base + j, n, stride=tiles), :] = value[:, j * LANES : (j + 1) * LANES]

    def spread_rows(base, n):
        return wide[pl.ds(base, n * tiles), :].reshape(n, tiles, LANES)

    spread(rows, 0)
    picked[...] = spread_rows(0, chips).astype(BF16)
    mine[chip] = picked[chip]

    pl.semaphore_wait(barrier, len(peers) + 1)

    def scatter(src, dst, send, recv):
        copies = []
        for j in peers:
            copy = pltpu.make_async_remote_copy(
                src_ref=src.at[j], dst_ref=dst.at[chip], send_sem=send.at[j], recv_sem=recv.at[chip],
                device_id={"ep": 2 * j + core}, device_id_type=MESH,
            )
            copy.start()
            copies.append(copy)
        return copies

    def arrival(dst, send, recv, j):
        return pltpu.make_async_remote_copy(
            src_ref=dst.at[j], dst_ref=dst.at[j], send_sem=send.at[j], recv_sem=recv.at[j],
            device_id=partner, device_id_type=MESH,
        )

    sent = scatter(picked, mine, send1, recv1)

    half = side // 2
    group = 2 * side
    order = sorted(range(half), key=lambda d: min(d, half - d))
    groups = [lax.rem(row // 2 + d, half) for d in order]

    def flatten(src, g, first):
        start = pl.multiple_of(g * group, group)
        place = pl.multiple_of(first + start, group)
        base = pl.multiple_of(place * tiles, group)
        wide[pl.ds(base, group * tiles), :] = src[pl.ds(start, group)].astype(F32).reshape(group * tiles, LANES)
        for j in range(used):
            lane_tile = wide[pl.ds(base + j, group, stride=tiles), :]
            arrived[pl.ds(place, group), j * LANES : (j + 1) * LANES] = lane_tile.astype(BF16)

    forwards = []
    for d, g in zip(order, groups):
        start = pl.multiple_of(g * group, group)
        for i in range(group):
            j = start + i

            if d == 0:
                @pl.when(j != chip)
                def _():
                    arrival(mine, send1, recv1, j).wait_recv()
            else:
                arrival(mine, send1, recv1, j).wait_recv()
        copy = pltpu.make_async_remote_copy(
            src_ref=mine.at[pl.ds(start, group)], dst_ref=other.at[pl.ds(start, group)],
            send_sem=send_x.at[g], recv_sem=recv_x.at[g], device_id=partner, device_id_type=MESH,
        )
        copy.start()
        forwards.append(copy)
        flatten(mine, g, 0)
    for copy, g in zip(forwards, groups):
        copy.wait_recv()
        flatten(other, g, chips)
    sent += forwards

    for copy in weights[:2]:
        copy.wait()
    rows_in = arrived[:, :width]
    gate_out = lax.dot_general(gate_v[...], rows_in, ROWS_BY_ROWS, preferred_element_type=F32)
    upward = lax.dot_general(up_v[...], rows_in, ROWS_BY_ROWS, preferred_element_type=F32)
    hidden = (gate_out / (1.0 + jnp.exp(-gate_out)) * upward).astype(BF16)
    weights[2].wait()
    pieces = given.shape[0]
    piece = given.shape[2]
    exchanges = []
    for i in range(pieces):
        low, size = i * piece, min(piece, width - i * piece)
        partial = lax.dot_general(
            hidden, down_v[:, low : low + size], COLUMNS_BY_ROWS, preferred_element_type=F32
        ).astype(BF16)
        given[i, :, :size] = partial[chips:]
        if size < piece:
            given[i, :, size:] = jnp.zeros((chips, piece - size), BF16)
        own_share[i, :, :size] = partial[:chips]
        copy = pltpu.make_async_remote_copy(
            src_ref=given.at[i], dst_ref=taken.at[i], send_sem=send_y.at[i], recv_sem=recv_y.at[i],
            device_id=partner, device_id_type=MESH,
        )
        copy.start()
        exchanges.append(copy)
    for i, copy in enumerate(exchanges):
        copy.wait_recv()
        size = min(piece, width - i * piece)
        total = own_share[i].astype(F32) + taken[i].astype(F32)
        for j in range(pl.cdiv(size, LANES)):
            wide[pl.ds(i * (piece // LANES) + j, chips, stride=tiles), :] = total[:, j * LANES : (j + 1) * LANES]
    sent += exchanges
    summed[...] = spread_rows(0, chips).astype(BF16)
    results[chip] = summed[chip]
    sent += scatter(summed, results, send2, recv2)
    for j in peers[::-1]:
        arrival(results, send2, recv2, j).wait_recv()

    for t in range(count):
        codes = [codes_s[k, t] for k in range(top)]
        mixture = sum(
            results[ids_s[k, t]].astype(F32) * codes[k].astype(F32) for k in range(top)
        )
        mixture = mixture / jnp.full(mixture.shape, sum(codes).astype(F32))
        wide[t * tiles : (t + 1) * tiles, :] = mixture
    for j in range(used):
        low, size = j * LANES, min(LANES, width - j * LANES)
        lane_tile = wide[pl.ds(j, count, stride=tiles), :]
        out_ref[:, low : low + size] = (
            tokens_v[:, low : low + size].astype(F32) + lane_tile[:, :size]
        ).astype(BF16)
    for copy in sent:
        copy.wait_send()


def shards(tokens, norm_gain, expert_ids, gate_codes, w_gate, w_up, w_down):
    side = math.isqrt(lax.axis_size("ep") // 2)
    chips = side * side
    count, width = tokens.shape
    shard_ff = w_gate.shape[2]
    tiles = 8 * pl.cdiv(width, 8 * LANES)
    pieces = 3
    piece = LANES * (tiles // pieces)
    blocks = pltpu.VMEM((chips, tiles, LANES), BF16)
    shares = pltpu.VMEM((pieces, chips, piece), BF16)
    DMA = pltpu.SemaphoreType.DMA
    return pl.pallas_call(
        functools.partial(kernel, side, tiles),
        out_shape=jax.ShapeDtypeStruct((count, width), BF16),
        in_specs=[pl.BlockSpec(memory_space=pl.ANY)] * 7,
        out_specs=pl.BlockSpec(memory_space=pltpu.VMEM),
        scratch_shapes=[
            pltpu.VMEM((count, width), BF16),
            pltpu.VMEM((width,), F32),
            pltpu.VMEM(expert_ids.shape[::-1], jnp.int32),
            pltpu.SMEM(expert_ids.shape[::-1], jnp.int32),
            pltpu.SMEM(gate_codes.shape[::-1], jnp.int32),
            pltpu.VMEM((shard_ff, width), BF16),
            pltpu.VMEM((shard_ff, width), BF16),
            pltpu.VMEM((shard_ff, width), BF16),
            pltpu.VMEM((2 * chips * tiles, LANES), F32),
            blocks,
            blocks,
            blocks,
            pltpu.VMEM((2 * chips, tiles * LANES), BF16),
            shares,
            shares,
            shares,
            blocks,
            blocks,
            DMA((5,)),
            DMA((3,)),
            DMA((chips,)),
            DMA((chips,)),
            DMA((side // 2,)),
            DMA((side // 2,)),
            DMA((pieces,)),
            DMA((pieces,)),
            DMA((chips,)),
            DMA((chips,)),
        ],
        compiler_params=pltpu.CompilerParams(
            collective_id=0, has_side_effects=True, vmem_limit_bytes=60 * 2**20
        ),
    )(
        tokens, norm_gain, expert_ids.T, gate_codes.T,
        jnp.swapaxes(w_gate, 1, 2), jnp.swapaxes(w_up, 1, 2), w_down,
    )


def solution(mesh):
    return jax.shard_map(
        shards,
        mesh=mesh,
        in_specs=(
            P(("groups", "ep"), None),
            P(),
            P(("groups", "ep"), None),
            P(("groups", "ep"), None),
            P("ep", None, None),
            P("ep", None, None),
            P("ep", None, None),
        ),
        out_specs=P(("groups", "ep"), None),
        check_vma=False,
    )
```

```python
import functools
import math

import jax
import jax.numpy as jnp
from jax import lax
from jax.experimental import pallas as pl
from jax.experimental.pallas import tpu as pltpu
from jax.sharding import PartitionSpec as P

epsilon = 1e-05
MESH = pl.DeviceIdType.MESH
F32 = jnp.float32
BF16 = jnp.bfloat16
LANES = 128
ROWS_BY_ROWS = (((1,), (1,)), ((), ()))
COLUMNS_BY_ROWS = (((0,), (0,)), ((), ()))


def kernel(
    side, tiles,
    tokens_hbm, gain_hbm, ids_hbm, codes_hbm, gate_hbm, up_hbm, down_hbm,
    out_ref,
    tokens_v, gain_v, ids_v, ids_s, codes_s, gate_v, up_v, down_v,
    wide, picked, mine, other, arrived, given, taken, own_share, summed, results,
    load_sem, weight_sem,
    send1, recv1, send_x, recv_x, send_y, recv_y, send2, recv2,
):
    me = lax.axis_index("ep")
    core = lax.rem(me, 2)
    chip = me // 2
    row, column = chip // side, lax.rem(chip, side)
    chips = side * side
    count, width = tokens_v.shape
    top = ids_v.shape[0]
    padded = tiles * LANES
    used = pl.cdiv(width, LANES)
    partner = {"ep": me + 1 - 2 * core}

    near = lambda d: min(d, side - d)
    offsets = [(dy, dx) for dy in range(side) for dx in range(side) if dy or dx]
    offsets.sort(key=lambda o: (-near(o[0]), -near(o[1])))
    rows_at = [lax.rem(row + d, side) for d in range(side)]
    columns_at = [lax.rem(column + d, side) for d in range(side)]
    first_at = [jnp.where(core == 0, r * side, c) for r, c in zip(rows_at, columns_at)]
    turned_first = [jnp.where(core == 0, column + d, (row + d)) for d in range(side)]
    second_at = [lax.rem(v, side) * jnp.where(core == 0, 1, side) for v in turned_first]
    peers = [first_at[a] + second_at[b] for a, b in offsets]

    small = [
        pltpu.make_async_copy(src, dst, load_sem.at[i])
        for i, (src, dst) in enumerate(
            [(tokens_hbm, tokens_v), (gain_hbm, gain_v), (ids_hbm, ids_v), (ids_hbm, ids_s), (codes_hbm, codes_s)]
        )
    ]
    for copy in small:
        copy.start()
    weights = [
        pltpu.make_async_copy(src.at[0], dst, weight_sem.at[i])
        for i, (src, dst) in enumerate([(gate_hbm, gate_v), (up_hbm, up_v), (down_hbm, down_v)])
    ]

    barrier = pltpu.get_barrier_semaphore()
    for j in peers:
        pl.semaphore_signal(barrier, inc=1, device_id={"ep": 2 * j + core}, device_id_type=MESH)
    pl.semaphore_signal(barrier, inc=1, device_id=partner, device_id_type=MESH)
    for copy in small:
        copy.wait()
    for copy in weights:
        copy.start()

    values = tokens_v[...].astype(F32)
    normed = values * lax.rsqrt(jnp.mean(values * values, axis=1, keepdims=True) + epsilon) * gain_v[...].reshape(1, -1)
    normed = normed.astype(BF16)
    expert = lax.broadcasted_iota(jnp.int32, (chips, count), 0)
    chosen = jnp.zeros(expert.shape, F32)
    for k in range(top):
        chosen = jnp.where(ids_v[k : k + 1, :] == expert, 1.0, chosen)
    rows = jnp.dot(chosen.astype(BF16), normed, preferred_element_type=F32)

    def spread(value, base):
        n = value.shape[0]
        value = jnp.concatenate([value, jnp.zeros((n, padded - width), F32)], axis=1)
        for j in range(tiles):
            wide[pl.ds(base + j, n, stride=tiles), :] = value[:, j * LANES : (j + 1) * LANES]

    def spread_rows(base, n):
        return wide[pl.ds(base, n * tiles), :].reshape(n, tiles, LANES)

    spread(rows, 0)
    picked[...] = spread_rows(0, chips).astype(BF16)
    mine[chip] = picked[chip]

    pl.semaphore_wait(barrier, len(peers) + 1)

    def scatter(src, dst, send, recv):
        copies = []
        for j in peers:
            copy = pltpu.make_async_remote_copy(
                src_ref=src.at[j], dst_ref=dst.at[chip], send_sem=send.at[j], recv_sem=recv.at[chip],
                device_id={"ep": 2 * j + core}, device_id_type=MESH,
            )
            copy.start()
            copies.append(copy)
        return copies

    def arrival(dst, send, recv, j):
        return pltpu.make_async_remote_copy(
            src_ref=dst.at[j], dst_ref=dst.at[j], send_sem=send.at[j], recv_sem=recv.at[j],
            device_id=partner, device_id_type=MESH,
        )

    sent = scatter(picked, mine, send1, recv1)

    half = side // 2
    group = 2 * side
    order = sorted(range(half), key=lambda d: min(d, half - d))
    groups = [lax.rem(row // 2 + d, half) for d in order]

    def flatten(src, g, first):
        start = pl.multiple_of(g * group, group)
        place = pl.multiple_of(first + start, group)
        base = pl.multiple_of(place * tiles, group)
        wide[pl.ds(base, group * tiles), :] = src[pl.ds(start, group)].astype(F32).reshape(group * tiles, LANES)
        for j in range(used):
            lane_tile = wide[pl.ds(base + j, group, stride=tiles), :]
            arrived[pl.ds(place, group), j * LANES : (j + 1) * LANES] = lane_tile.astype(BF16)

    forwards = []

    def flatten_other():
        i = len(forwards) - 1
        forwards[i].wait_recv()
        flatten(other, groups[i], chips)

    for d, g in zip(order, groups):
        start = pl.multiple_of(g * group, group)
        for i in range(group):
            j = start + i

            if d == 0:
                @pl.when(j != chip)
                def _():
                    arrival(mine, send1, recv1, j).wait_recv()
            else:
                arrival(mine, send1, recv1, j).wait_recv()
        copy = pltpu.make_async_remote_copy(
            src_ref=mine.at[pl.ds(start, group)], dst_ref=other.at[pl.ds(start, group)],
            send_sem=send_x.at[g], recv_sem=recv_x.at[g], device_id=partner, device_id_type=MESH,
        )
        copy.start()
        if forwards:
            flatten_other()
        forwards.append(copy)
        flatten(mine, g, 0)
    flatten_other()
    sent += forwards

    for copy in weights[:2]:
        copy.wait()
    rows_in = arrived[:, :width]
    gate_out = lax.dot_general(gate_v[...], rows_in, ROWS_BY_ROWS, preferred_element_type=F32)
    upward = lax.dot_general(up_v[...], rows_in, ROWS_BY_ROWS, preferred_element_type=F32)
    hidden = (gate_out / (1.0 + jnp.exp(-gate_out)) * upward).astype(BF16)
    weights[2].wait()
    pieces = given.shape[0]
    piece = given.shape[2]
    exchanges = []
    for i in range(pieces):
        low, size = i * piece, min(piece, width - i * piece)
        partial = lax.dot_general(
            hidden, down_v[:, low : low + size], COLUMNS_BY_ROWS, preferred_element_type=F32
        ).astype(BF16)
        given[i, :, :size] = partial[chips:]
        if size < piece:
            given[i, :, size:] = jnp.zeros((chips, piece - size), BF16)
        own_share[i, :, :size] = partial[:chips]
        copy = pltpu.make_async_remote_copy(
            src_ref=given.at[i], dst_ref=taken.at[i], send_sem=send_y.at[i], recv_sem=recv_y.at[i],
            device_id=partner, device_id_type=MESH,
        )
        copy.start()
        exchanges.append(copy)
    for i, copy in enumerate(exchanges):
        copy.wait_recv()
        size = min(piece, width - i * piece)
        total = own_share[i].astype(F32) + taken[i].astype(F32)
        for j in range(pl.cdiv(size, LANES)):
            wide[pl.ds(i * (piece // LANES) + j, chips, stride=tiles), :] = total[:, j * LANES : (j + 1) * LANES]
    sent += exchanges
    summed[...] = spread_rows(0, chips).astype(BF16)
    results[chip] = summed[chip]
    sent += scatter(summed, results, send2, recv2)
    for j in peers[::-1]:
        arrival(results, send2, recv2, j).wait_recv()

    for t in range(count):
        codes = [codes_s[k, t] for k in range(top)]
        mixture = sum(
            results[ids_s[k, t]].astype(F32) * codes[k].astype(F32) for k in range(top)
        )
        mixture = mixture / jnp.full(mixture.shape, sum(codes).astype(F32))
        wide[t * tiles : (t + 1) * tiles, :] = mixture
    for j in range(used):
        low, size = j * LANES, min(LANES, width - j * LANES)
        lane_tile = wide[pl.ds(j, count, stride=tiles), :]
        out_ref[:, low : low + size] = (
            tokens_v[:, low : low + size].astype(F32) + lane_tile[:, :size]
        ).astype(BF16)
    for copy in sent:
        copy.wait_send()


def shards(tokens, norm_gain, expert_ids, gate_codes, w_gate, w_up, w_down):
    side = math.isqrt(lax.axis_size("ep") // 2)
    chips = side * side
    count, width = tokens.shape
    shard_ff = w_gate.shape[2]
    tiles = 8 * pl.cdiv(width, 8 * LANES)
    pieces = 3
    piece = LANES * (tiles // pieces)
    blocks = pltpu.VMEM((chips, tiles, LANES), BF16)
    shares = pltpu.VMEM((pieces, chips, piece), BF16)
    DMA = pltpu.SemaphoreType.DMA
    return pl.pallas_call(
        functools.partial(kernel, side, tiles),
        out_shape=jax.ShapeDtypeStruct((count, width), BF16),
        in_specs=[pl.BlockSpec(memory_space=pltpu.HBM)] * 7,
        out_specs=pl.BlockSpec(memory_space=pltpu.VMEM),
        scratch_shapes=[
            pltpu.VMEM((count, width), BF16),
            pltpu.VMEM((width,), F32),
            pltpu.VMEM(expert_ids.shape[::-1], jnp.int32),
            pltpu.SMEM(expert_ids.shape[::-1], jnp.int32),
            pltpu.SMEM(gate_codes.shape[::-1], jnp.int32),
            pltpu.VMEM((shard_ff, width), BF16),
            pltpu.VMEM((shard_ff, width), BF16),
            pltpu.VMEM((shard_ff, width), BF16),
            pltpu.VMEM((2 * chips * tiles, LANES), F32),
            blocks,
            blocks,
            blocks,
            pltpu.VMEM((2 * chips, tiles * LANES), BF16),
            shares,
            shares,
            shares,
            blocks,
            blocks,
            DMA((5,)),
            DMA((3,)),
            DMA((chips,)),
            DMA((chips,)),
            DMA((side // 2,)),
            DMA((side // 2,)),
            DMA((pieces,)),
            DMA((pieces,)),
            DMA((chips,)),
            DMA((chips,)),
        ],
        compiler_params=pltpu.CompilerParams(
            collective_id=0, has_side_effects=True, vmem_limit_bytes=28 * 2**20
        ),
    )(*[
        pltpu.with_memory_space_constraint(array, pltpu.HBM)
        for array in (
            tokens, norm_gain, expert_ids.T, gate_codes.T,
            jnp.swapaxes(w_gate, 1, 2), jnp.swapaxes(w_up, 1, 2), w_down,
        )
    ])


def solution(mesh):
    return jax.shard_map(
        shards,
        mesh=mesh,
        in_specs=(
            P(("groups", "ep"), None),
            P(),
            P(("groups", "ep"), None),
            P(("groups", "ep"), None),
            P("ep", None, None),
            P("ep", None, None),
            P("ep", None, None),
        ),
        out_specs=P(("groups", "ep"), None),
        check_vma=False,
    )
```

```python
import functools
import math

import jax
import jax.numpy as jnp
from jax import lax
from jax.experimental import pallas as pl
from jax.experimental.pallas import tpu as pltpu
from jax.sharding import PartitionSpec as P

epsilon = 1e-05
MESH = pl.DeviceIdType.MESH
F32 = jnp.float32
BF16 = jnp.bfloat16
LANES = 128
ROWS_BY_ROWS = (((1,), (1,)), ((), ()))
COLUMNS_BY_ROWS = (((0,), (0,)), ((), ()))


def kernel(
    side, tiles,
    tokens_hbm, gain_hbm, ids_hbm, codes_hbm, gate_hbm, up_hbm, down_hbm,
    out_ref,
    tokens_v, gain_v, ids_v, ids_s, codes_s, gate_v, up_v, down_v,
    wide, picked, mine, other, arrived, given, taken, own_share, summed, results,
    load_sem, weight_sem,
    send1, recv1, send_x, recv_x, send_y, recv_y, send2, recv2,
):
    me = lax.axis_index("ep")
    core = lax.rem(me, 2)
    chip = me // 2
    row, column = chip // side, lax.rem(chip, side)
    chips = side * side
    count, width = tokens_v.shape
    top = ids_v.shape[0]
    padded = tiles * LANES
    used = pl.cdiv(width, LANES)
    partner = {"ep": me + 1 - 2 * core}

    near = lambda d: min(d, side - d)
    offsets = [(dy, dx) for dy in range(side) for dx in range(side) if dy or dx]
    rows_at = [lax.rem(row + d, side) for d in range(side)]
    columns_at = [lax.rem(column + d, side) for d in range(side)]
    offsets.sort(key=lambda o: -(near(o[0]) + near(o[1])))
    peers_out = [rows_at[dy] * side + columns_at[dx] for dy, dx in offsets]
    offsets.sort(key=lambda o: (-near(o[0]), -near(o[1])))
    major = [jnp.where(core == 0, r * side, c) for r, c in zip(rows_at, columns_at)]
    minor = [jnp.where(core == 0, c, r * side) for r, c in zip(rows_at, columns_at)]
    peers_back = [major[i] + minor[j] for i, j in offsets]

    small = [
        pltpu.make_async_copy(src, dst, load_sem.at[i])
        for i, (src, dst) in enumerate(
            [(tokens_hbm, tokens_v), (gain_hbm, gain_v), (ids_hbm, ids_v), (ids_hbm, ids_s), (codes_hbm, codes_s)]
        )
    ]
    for copy in small:
        copy.start()
    weights = [
        pltpu.make_async_copy(src.at[0], dst, weight_sem.at[i])
        for i, (src, dst) in enumerate([(gate_hbm, gate_v), (up_hbm, up_v), (down_hbm, down_v)])
    ]

    barrier = pltpu.get_barrier_semaphore()
    for j in peers_out:
        pl.semaphore_signal(barrier, inc=1, device_id={"ep": 2 * j + core}, device_id_type=MESH)
    pl.semaphore_signal(barrier, inc=1, device_id=partner, device_id_type=MESH)
    for copy in small:
        copy.wait()
    for copy in weights:
        copy.start()

    values = tokens_v[...].astype(F32)
    normed = values * lax.rsqrt(jnp.mean(values * values, axis=1, keepdims=True) + epsilon) * gain_v[...].reshape(1, -1)
    normed = normed.astype(BF16)
    expert = lax.broadcasted_iota(jnp.int32, (chips, count), 0)
    chosen = jnp.zeros(expert.shape, F32)
    for k in range(top):
        chosen = jnp.where(ids_v[k : k + 1, :] == expert, 1.0, chosen)
    rows = jnp.dot(chosen.astype(BF16), normed, preferred_element_type=F32)

    def spread(value, base):
        n = value.shape[0]
        value = jnp.concatenate([value, jnp.zeros((n, padded - width), F32)], axis=1)
        for j in range(tiles):
            wide[pl.ds(base + j, n, stride=tiles), :] = value[:, j * LANES : (j + 1) * LANES]

    def spread_rows(base, n):
        return wide[pl.ds(base, n * tiles), :].reshape(n, tiles, LANES)

    spread(rows, 0)
    picked[...] = spread_rows(0, chips).astype(BF16)
    mine[chip] = picked[chip]

    pl.semaphore_wait(barrier, len(peers_out) + 1)

    def scatter(peers, src, dst, send, recv):
        copies = []
        for j in peers:
            copy = pltpu.make_async_remote_copy(
                src_ref=src.at[j], dst_ref=dst.at[chip], send_sem=send.at[j], recv_sem=recv.at[chip],
                device_id={"ep": 2 * j + core}, device_id_type=MESH,
            )
            copy.start()
            copies.append(copy)
        return copies

    def arrival(dst, send, recv, j):
        return pltpu.make_async_remote_copy(
            src_ref=dst.at[j], dst_ref=dst.at[j], send_sem=send.at[j], recv_sem=recv.at[j],
            device_id=partner, device_id_type=MESH,
        )

    sent = scatter(peers_out, picked, mine, send1, recv1)

    half = side // 2
    group = 2 * side
    order = sorted(range(half), key=lambda d: min(d, half - d))
    groups = [lax.rem(row // 2 + d, half) for d in order]

    def flatten(src, g, first):
        start = pl.multiple_of(g * group, group)
        place = pl.multiple_of(first + start, group)
        base = pl.multiple_of(place * tiles, group)
        wide[pl.ds(base, group * tiles), :] = src[pl.ds(start, group)].astype(F32).reshape(group * tiles, LANES)
        for j in range(used):
            lane_tile = wide[pl.ds(base + j, group, stride=tiles), :]
            arrived[pl.ds(place, group), j * LANES : (j + 1) * LANES] = lane_tile.astype(BF16)

    forwards = []

    def flatten_other():
        i = len(forwards) - 1
        forwards[i].wait_recv()
        flatten(other, groups[i], chips)

    for d, g in zip(order, groups):
        start = pl.multiple_of(g * group, group)
        for i in range(group):
            j = start + i

            if d == 0:
                @pl.when(j != chip)
                def _():
                    arrival(mine, send1, recv1, j).wait_recv()
            else:
                arrival(mine, send1, recv1, j).wait_recv()
        copy = pltpu.make_async_remote_copy(
            src_ref=mine.at[pl.ds(start, group)], dst_ref=other.at[pl.ds(start, group)],
            send_sem=send_x.at[g], recv_sem=recv_x.at[g], device_id=partner, device_id_type=MESH,
        )
        copy.start()
        if forwards:
            flatten_other()
        forwards.append(copy)
        flatten(mine, g, 0)
    flatten_other()
    sent += forwards

    for copy in weights[:2]:
        copy.wait()
    rows_in = arrived[:, :width]
    gate_out = lax.dot_general(gate_v[...], rows_in, ROWS_BY_ROWS, preferred_element_type=F32)
    upward = lax.dot_general(up_v[...], rows_in, ROWS_BY_ROWS, preferred_element_type=F32)
    hidden = (gate_out / (1.0 + jnp.exp(-gate_out)) * upward).astype(BF16)
    weights[2].wait()
    pieces = given.shape[0]
    piece = given.shape[2]
    exchanges = []
    for i in range(pieces):
        low, size = i * piece, min(piece, width - i * piece)
        partial = lax.dot_general(
            hidden, down_v[:, low : low + size], COLUMNS_BY_ROWS, preferred_element_type=F32
        ).astype(BF16)
        given[i, :, :size] = partial[chips:]
        if size < piece:
            given[i, :, size:] = jnp.zeros((chips, piece - size), BF16)
        own_share[i, :, :size] = partial[:chips]
        copy = pltpu.make_async_remote_copy(
            src_ref=given.at[i], dst_ref=taken.at[i], send_sem=send_y.at[i], recv_sem=recv_y.at[i],
            device_id=partner, device_id_type=MESH,
        )
        copy.start()
        exchanges.append(copy)
    for i, copy in enumerate(exchanges):
        copy.wait_recv()
        size = min(piece, width - i * piece)
        total = own_share[i].astype(F32) + taken[i].astype(F32)
        for j in range(pl.cdiv(size, LANES)):
            wide[pl.ds(i * (piece // LANES) + j, chips, stride=tiles), :] = total[:, j * LANES : (j + 1) * LANES]
    sent += exchanges
    summed[...] = spread_rows(0, chips).astype(BF16)
    results[chip] = summed[chip]
    sent += scatter(peers_back, summed, results, send2, recv2)
    for j in peers_back[::-1]:
        arrival(results, send2, recv2, j).wait_recv()

    for t in range(count):
        codes = [codes_s[k, t] for k in range(top)]
        mixture = sum(
            results[ids_s[k, t]].astype(F32) * codes[k].astype(F32) for k in range(top)
        )
        mixture = mixture / jnp.full(mixture.shape, sum(codes).astype(F32))
        wide[t * tiles : (t + 1) * tiles, :] = mixture
    for j in range(used):
        low, size = j * LANES, min(LANES, width - j * LANES)
        lane_tile = wide[pl.ds(j, count, stride=tiles), :]
        out_ref[:, low : low + size] = (
            tokens_v[:, low : low + size].astype(F32) + lane_tile[:, :size]
        ).astype(BF16)
    for copy in sent:
        copy.wait_send()


def shards(tokens, norm_gain, expert_ids, gate_codes, w_gate, w_up, w_down):
    side = math.isqrt(lax.axis_size("ep") // 2)
    chips = side * side
    count, width = tokens.shape
    shard_ff = w_gate.shape[2]
    tiles = 8 * pl.cdiv(width, 8 * LANES)
    pieces = 3
    piece = LANES * (tiles // pieces)
    blocks = pltpu.VMEM((chips, tiles, LANES), BF16)
    shares = pltpu.VMEM((pieces, chips, piece), BF16)
    DMA = pltpu.SemaphoreType.DMA
    return pl.pallas_call(
        functools.partial(kernel, side, tiles),
        out_shape=jax.ShapeDtypeStruct((count, width), BF16),
        in_specs=[pl.BlockSpec(memory_space=pltpu.HBM)] * 7,
        out_specs=pl.BlockSpec(memory_space=pltpu.VMEM),
        scratch_shapes=[
            pltpu.VMEM((count, width), BF16),
            pltpu.VMEM((width,), F32),
            pltpu.VMEM(expert_ids.shape[::-1], jnp.int32),
            pltpu.SMEM(expert_ids.shape[::-1], jnp.int32),
            pltpu.SMEM(gate_codes.shape[::-1], jnp.int32),
            pltpu.VMEM((shard_ff, width), BF16),
            pltpu.VMEM((shard_ff, width), BF16),
            pltpu.VMEM((shard_ff, width), BF16),
            pltpu.VMEM((2 * chips * tiles, LANES), F32),
            blocks,
            blocks,
            blocks,
            pltpu.VMEM((2 * chips, tiles * LANES), BF16),
            shares,
            shares,
            shares,
            blocks,
            blocks,
            DMA((5,)),
            DMA((3,)),
            DMA((chips,)),
            DMA((chips,)),
            DMA((side // 2,)),
            DMA((side // 2,)),
            DMA((pieces,)),
            DMA((pieces,)),
            DMA((chips,)),
            DMA((chips,)),
        ],
        compiler_params=pltpu.CompilerParams(
            collective_id=0, has_side_effects=True, vmem_limit_bytes=28 * 2**20
        ),
    )(*[
        pltpu.with_memory_space_constraint(array, pltpu.HBM)
        for array in (
            tokens, norm_gain, expert_ids.T, gate_codes.T,
            jnp.swapaxes(w_gate, 1, 2), jnp.swapaxes(w_up, 1, 2), w_down,
        )
    ])


def solution(mesh):
    return jax.shard_map(
        shards,
        mesh=mesh,
        in_specs=(
            P(("groups", "ep"), None),
            P(),
            P(("groups", "ep"), None),
            P(("groups", "ep"), None),
            P("ep", None, None),
            P("ep", None, None),
            P("ep", None, None),
        ),
        out_specs=P(("groups", "ep"), None),
        check_vma=False,
    )
```

```python
import functools
import math

import jax
import jax.numpy as jnp
from jax import lax
from jax.experimental import pallas as pl
from jax.experimental.pallas import tpu as pltpu
from jax.sharding import PartitionSpec as P

epsilon = 1e-05
MESH = pl.DeviceIdType.MESH
F32 = jnp.float32
BF16 = jnp.bfloat16
LANES = 128


def kernel(
    side, tiles,
    tokens_hbm, gain_hbm, ids_hbm, codes_hbm, gate_hbm, up_hbm, down_hbm,
    out_ref,
    tokens_v, gain_v, ids_v, ids_s, codes_s, gate_v, up_v, down_v, gate_t, up_t,
    picked, slots, arrived, share, taken, summed, results,
    load_sem, weight_sem, ready,
    send1, recv1, send_x, recv_x, send_y, recv_y, send2, recv2,
):
    me = lax.axis_index("ep")
    core = lax.rem(me, 2)
    chip = me // 2
    row, column = chip // side, lax.rem(chip, side)
    chips = side * side
    count, width = tokens_v.shape
    top = ids_v.shape[0]
    padded = tiles * LANES
    partner = {"ep": me + 1 - 2 * core}

    near = lambda d: min(d, side - d)
    offsets = [(dy, dx) for dy in range(side) for dx in range(side) if dy or dx]
    rows_at = [lax.rem(row + d, side) * side for d in range(side)]
    columns_at = [lax.rem(column + d, side) for d in range(side)]
    offsets.sort(key=lambda o: -(near(o[0]) + near(o[1])))
    peers = [rows_at[dy] + columns_at[dx] for dy, dx in offsets]

    small = [
        pltpu.make_async_copy(src, dst, load_sem.at[i])
        for i, (src, dst) in enumerate(
            [(tokens_hbm, tokens_v), (gain_hbm, gain_v), (ids_hbm, ids_v), (ids_hbm, ids_s), (codes_hbm, codes_s)]
        )
    ]
    for copy in small:
        copy.start()
    weights = [
        pltpu.make_async_copy(src.at[0], dst, weight_sem.at[i])
        for i, (src, dst) in enumerate([(gate_hbm, gate_v), (up_hbm, up_v), (down_hbm, down_v)])
    ]

    barrier = pltpu.get_barrier_semaphore()
    for j in peers:
        pl.semaphore_signal(barrier, inc=1, device_id={"ep": 2 * j + core}, device_id_type=MESH)

    @pl.when(core == 1)
    def _():
        pl.semaphore_signal(barrier, inc=1, device_id=partner, device_id_type=MESH)

    for copy in small:
        copy.wait()
    for copy in weights:
        copy.start()

    values = tokens_v[...].astype(F32)
    normed = values * lax.rsqrt(jnp.mean(values * values, axis=1, keepdims=True) + epsilon) * gain_v[...].reshape(1, -1)
    normed = normed.astype(BF16)
    expert = lax.broadcasted_iota(jnp.int32, (chips, count), 0)
    chosen = jnp.zeros(expert.shape, F32)
    for k in range(top):
        chosen = jnp.where(ids_v[k : k + 1, :] == expert, 1.0, chosen)
    rows = jnp.dot(chosen.astype(BF16), normed, preferred_element_type=F32)
    rows = jnp.concatenate([rows, jnp.zeros((chips, padded - width), F32)], axis=1)
    picked[...] = rows.reshape(picked.shape).astype(BF16)
    slots[core, chip] = picked[chip]

    pl.semaphore_wait(barrier, len(peers) + 1 - core)

    @pl.when(core == 0)
    def _():
        pl.semaphore_signal(ready, inc=1, device_id=partner, device_id_type=MESH)

    def scatter(src, dst, send, recv):
        for j in peers:
            pltpu.make_async_remote_copy(
                src_ref=src.at[j], dst_ref=dst.at[chip], send_sem=send.at[j], recv_sem=recv.at[chip],
                device_id={"ep": 2 * j + core}, device_id_type=MESH,
            ).start()

    def transfer(src, dst, send, recv):
        return pltpu.make_async_remote_copy(
            src_ref=src, dst_ref=dst, send_sem=send, recv_sem=recv, device_id=partner, device_id_type=MESH,
        )

    scatter(picked, slots.at[core], send1, recv1)

    depth = gate_t.shape[1]
    hidden_size = gate_v.shape[0]
    for i, (src, dst) in enumerate([(gate_v, gate_t), (up_v, up_t)]):
        weights[i].wait()
        dst[:, hidden_size:] = jnp.zeros((dst.shape[0], depth - hidden_size), BF16)
        for low in range(0, width, LANES):
            size = min(LANES, width - low)
            dst[low : low + size, :hidden_size] = src[:, low : low + size].T
        dst[width:, :] = jnp.zeros((dst.shape[0] - width, depth), BF16)

    half = side // 2
    group = 2 * side
    pieces, _, piece = share.shape[1:]
    sizes = [min(piece, width - i * piece) for i in range(pieces)]
    groups = [lax.rem(row // 2 + d, half) for d in sorted(range(half), key=lambda d: min(d, half - d))]

    def forward(plane, g):
        block = slots.at[plane, pl.ds(g * group, group)]
        return transfer(block, block, send_x.at[g], recv_x.at[g])

    def exchange(plane, i):
        return transfer(share.at[plane, i], taken.at[i], send_y.at[i], recv_y.at[i])

    def receive(plane):
        @pl.when(core == plane)
        def _():
            if plane == 1:
                pl.semaphore_wait(ready, 1)
            for n, g in enumerate(groups):
                for i in range(group):
                    j = g * group + i
                    block = slots.at[plane, j]

                    def arrive():
                        transfer(block, block, send1.at[j], recv1.at[j]).wait_recv()

                    if n == 0:
                        pl.when(j != chip)(arrive)
                    else:
                        arrive()
                forward(plane, g).start()

    for plane in (1, 0):
        receive(plane)

        @pl.when(core != plane)
        def _():
            for g in groups:
                forward(plane, g).wait_recv()

        arrived[...] = slots[plane].reshape(chips, padded)
        rows_in = arrived[:, : gate_t.shape[0]]
        gate_out = jnp.dot(rows_in, gate_t[...], preferred_element_type=F32)
        upward = jnp.dot(rows_in, up_t[...], preferred_element_type=F32)
        hidden = (gate_out / (1.0 + jnp.exp(-gate_out)) * upward).astype(BF16)[:, :hidden_size]
        if plane == 1:
            weights[2].wait()
        for i, size in enumerate(sizes):
            low = i * piece
            partial = jnp.dot(
                hidden, down_v[:, low : low + size], preferred_element_type=F32
            ).astype(BF16)
            if size < piece:
                partial = jnp.concatenate([partial, jnp.zeros((chips, piece - size), BF16)], axis=1)
            share[plane, i] = partial

            @pl.when(core != plane)
            def _():
                exchange(plane, i).start()

        @pl.when(core == plane)
        def _():
            for i in range(pieces):
                exchange(plane, i).wait_recv()
                total = share[plane, i].astype(F32) + taken[i].astype(F32)
                first = i * (piece // LANES)
                summed[:, first : first + piece // LANES, :] = total.reshape(
                    chips, piece // LANES, LANES
                ).astype(BF16)
            results[chip] = summed[chip]
            scatter(summed, results, send2, recv2)

    for j in peers[::-1]:
        transfer(results.at[j], results.at[j], send2.at[j], recv2.at[j]).wait_recv()

    mixtures = []
    for t in range(count):
        codes = [codes_s[k, t] for k in range(top)]
        mixture = sum(
            results[ids_s[k, t]].astype(F32) * codes[k].astype(F32) for k in range(top)
        )
        mixtures.append(mixture / jnp.full(mixture.shape, sum(codes).astype(F32)))
    mixture = jnp.stack(mixtures).reshape(count, padded)[:, :width]
    out_ref[...] = (tokens_v[...].astype(F32) + mixture).astype(BF16)

    for j in peers:
        transfer(picked.at[j], picked.at[j], send1.at[j], recv1.at[j]).wait_send()
        transfer(summed.at[j], summed.at[j], send2.at[j], recv2.at[j]).wait_send()
    for g in range(half):
        forward(core, g).wait_send()
    for i in range(pieces):
        exchange(1 - core, i).wait_send()


def shards(tokens, norm_gain, expert_ids, gate_codes, w_gate, w_up, w_down):
    side = math.isqrt(lax.axis_size("ep") // 2)
    chips = side * side
    count, width = tokens.shape
    shard_ff = w_gate.shape[2]
    tiles = 8 * pl.cdiv(width, 8 * LANES)
    pieces = 3
    piece = LANES * (tiles // pieces)
    blocks = pltpu.VMEM((chips, tiles, LANES), BF16)
    turned = pltpu.VMEM((LANES * pl.cdiv(width, LANES), 2 * LANES * pl.cdiv(shard_ff, 2 * LANES)), BF16)
    shares = (pieces, chips, piece)
    DMA = pltpu.SemaphoreType.DMA
    return pl.pallas_call(
        functools.partial(kernel, side, tiles),
        out_shape=jax.ShapeDtypeStruct((count, width), BF16),
        in_specs=[pl.BlockSpec(memory_space=pltpu.HBM)] * 7,
        out_specs=pl.BlockSpec(memory_space=pltpu.VMEM),
        scratch_shapes=[
            pltpu.VMEM((count, width), BF16),
            pltpu.VMEM((width,), F32),
            pltpu.VMEM(expert_ids.shape[::-1], jnp.int32),
            pltpu.SMEM(expert_ids.shape[::-1], jnp.int32),
            pltpu.SMEM(gate_codes.shape[::-1], jnp.int32),
            pltpu.VMEM((shard_ff, width), BF16),
            pltpu.VMEM((shard_ff, width), BF16),
            pltpu.VMEM((shard_ff, width), BF16),
            turned,
            turned,
            blocks,
            pltpu.VMEM((2, chips, tiles, LANES), BF16),
            pltpu.VMEM((chips, tiles * LANES), BF16),
            pltpu.VMEM((2,) + shares, BF16),
            pltpu.VMEM(shares, BF16),
            blocks,
            blocks,
            DMA((5,)),
            DMA((3,)),
            pltpu.SemaphoreType.REGULAR,
            DMA((chips,)),
            DMA((chips,)),
            DMA((side // 2,)),
            DMA((side // 2,)),
            DMA((pieces,)),
            DMA((pieces,)),
            DMA((chips,)),
            DMA((chips,)),
        ],
        compiler_params=pltpu.CompilerParams(
            collective_id=0, has_side_effects=True, vmem_limit_bytes=44 * 2**20
        ),
    )(*[
        pltpu.with_memory_space_constraint(array, pltpu.HBM)
        for array in (
            tokens, norm_gain, expert_ids.T, gate_codes.T,
            jnp.swapaxes(w_gate, 1, 2), jnp.swapaxes(w_up, 1, 2), w_down,
        )
    ])


def solution(mesh):
    return jax.shard_map(
        shards,
        mesh=mesh,
        in_specs=(
            P(("groups", "ep"), None),
            P(),
            P(("groups", "ep"), None),
            P(("groups", "ep"), None),
            P("ep", None, None),
            P("ep", None, None),
            P("ep", None, None),
        ),
        out_specs=P(("groups", "ep"), None),
        check_vma=False,
    )
```

```python
import functools
import math

import jax
import jax.numpy as jnp
from jax import lax
from jax.experimental import pallas as pl
from jax.experimental.pallas import tpu as pltpu
from jax.sharding import PartitionSpec as P

epsilon = 1e-05
MESH = pl.DeviceIdType.MESH
F32 = jnp.float32
BF16 = jnp.bfloat16
LANES = 128


def kernel(
    side, tiles,
    tokens_hbm, gain_hbm, ids_hbm, codes_hbm, gate_hbm, up_hbm, down_hbm,
    out_ref,
    tokens_v, gain_v, ids_v, ids_s, codes_s, gate_v, up_v, down_v, gate_t, up_t,
    picked, slots, arrived, share, taken, summed, results,
    load_sem, weight_sem, ready,
    send1, recv1, send_x, recv_x, send_y, recv_y, send2, recv2,
):
    me = lax.axis_index("ep")
    core = lax.rem(me, 2)
    chip = me // 2
    row, column = chip // side, lax.rem(chip, side)
    chips = side * side
    count, width = tokens_v.shape
    top = ids_v.shape[0]
    padded = tiles * LANES
    partner = {"ep": me + 1 - 2 * core}

    near = lambda d: min(d, side - d)
    offsets = [(dy, dx) for dy in range(side) for dx in range(side) if dy or dx]
    rows_at = [lax.rem(row + d, side) * side for d in range(side)]
    columns_at = [lax.rem(column + d, side) for d in range(side)]
    offsets.sort(key=lambda o: -(near(o[0]) + near(o[1])))
    peers = [rows_at[dy] + columns_at[dx] for dy, dx in offsets]

    barrier = pltpu.get_barrier_semaphore()
    for j in peers:
        pl.semaphore_signal(barrier, inc=1, device_id={"ep": 2 * j + core}, device_id_type=MESH)

    @pl.when(core == 1)
    def _():
        pl.semaphore_signal(barrier, inc=1, device_id=partner, device_id_type=MESH)

    small = [
        pltpu.make_async_copy(src, dst, load_sem.at[i])
        for i, (src, dst) in enumerate(
            [(tokens_hbm, tokens_v), (gain_hbm, gain_v), (ids_hbm, ids_v), (ids_hbm, ids_s), (codes_hbm, codes_s)]
        )
    ]
    for copy in small:
        copy.start()
    weights = [
        pltpu.make_async_copy(src.at[0], dst, weight_sem.at[i])
        for i, (src, dst) in enumerate([(gate_hbm, gate_v), (up_hbm, up_v), (down_hbm, down_v)])
    ]

    for copy in small:
        copy.wait()
    for copy in weights:
        copy.start()

    values = tokens_v[...].astype(F32)
    normed = values * lax.rsqrt(jnp.mean(values * values, axis=1, keepdims=True) + epsilon) * gain_v[...].reshape(1, -1)
    normed = normed.astype(BF16)
    expert = lax.broadcasted_iota(jnp.int32, (chips, count), 0)
    chosen = jnp.zeros(expert.shape, F32)
    for k in range(top):
        chosen = jnp.where(ids_v[k : k + 1, :] == expert, 1.0, chosen)
    rows = jnp.dot(chosen.astype(BF16), normed, preferred_element_type=F32)
    rows = jnp.concatenate([rows, jnp.zeros((chips, padded - width), F32)], axis=1)
    picked[...] = rows.reshape(picked.shape).astype(BF16)
    slots[core, chip] = picked[chip]

    pl.semaphore_wait(barrier, len(peers) + 1 - core)

    @pl.when(core == 0)
    def _():
        pl.semaphore_signal(ready, inc=1, device_id=partner, device_id_type=MESH)

    def scatter(src, dst, send, recv, chips_to, core_to):
        for j in chips_to:
            pltpu.make_async_remote_copy(
                src_ref=src.at[j], dst_ref=dst.at[chip], send_sem=send.at[j], recv_sem=recv.at[chip],
                device_id={"ep": 2 * j + core_to}, device_id_type=MESH,
            ).start()

    def transfer(src, dst, send, recv):
        return pltpu.make_async_remote_copy(
            src_ref=src, dst_ref=dst, send_sem=send, recv_sem=recv, device_id=partner, device_id_type=MESH,
        )

    scatter(picked, slots.at[core], send1, recv1, peers, core)

    depth = gate_t.shape[1]
    hidden_size = gate_v.shape[0]
    for i, (src, dst) in enumerate([(gate_v, gate_t), (up_v, up_t)]):
        weights[i].wait()
        dst[:, hidden_size:] = jnp.zeros((dst.shape[0], depth - hidden_size), BF16)
        for low in range(0, width, LANES):
            size = min(LANES, width - low)
            dst[low : low + size, :hidden_size] = src[:, low : low + size].T
        dst[width:, :] = jnp.zeros((dst.shape[0] - width, depth), BF16)

    half = side // 2
    group = 2 * side
    pieces, _, piece = share.shape[1:]
    sizes = [min(piece, width - i * piece) for i in range(pieces)]
    groups = [lax.rem(row // 2 + d, half) for d in sorted(range(half), key=lambda d: min(d, half - d))]

    def forward(plane, g):
        block = slots.at[plane, pl.ds(g * group, group)]
        return transfer(block, block, send_x.at[g], recv_x.at[g])

    def exchange(plane, i):
        return transfer(share.at[plane, i], taken.at[i], send_y.at[i], recv_y.at[i])

    def receive(plane):
        @pl.when(core == plane)
        def _():
            if plane == 1:
                pl.semaphore_wait(ready, 1)
            for n, g in enumerate(groups):
                for i in range(group):
                    j = g * group + i
                    block = slots.at[plane, j]

                    def arrive():
                        transfer(block, block, send1.at[j], recv1.at[j]).wait_recv()

                    if n == 0:
                        pl.when(j != chip)(arrive)
                    else:
                        arrive()
                forward(plane, g).start()

    for plane in (1, 0):
        receive(plane)

        @pl.when(core != plane)
        def _():
            for g in groups:
                forward(plane, g).wait_recv()

        arrived[...] = slots[plane].reshape(chips, padded)
        rows_in = arrived[:, : gate_t.shape[0]]
        gate_out = jnp.dot(rows_in, gate_t[...], preferred_element_type=F32)
        upward = jnp.dot(rows_in, up_t[...], preferred_element_type=F32)
        hidden = (gate_out / (1.0 + jnp.exp(-gate_out)) * upward).astype(BF16)[:, :hidden_size]
        if plane == 1:
            weights[2].wait()
        for i, size in enumerate(sizes):
            low = i * piece
            partial = jnp.dot(
                hidden, down_v[:, low : low + size], preferred_element_type=F32
            ).astype(BF16)
            if size < piece:
                partial = jnp.concatenate([partial, jnp.zeros((chips, piece - size), BF16)], axis=1)
            share[plane, i] = partial

            @pl.when(core == plane)
            def _():
                exchange(plane, i).start()

        @pl.when(core != plane)
        def _():
            for i in range(pieces):
                exchange(plane, i).wait_recv()
                total = share[plane, i].astype(F32) + taken[i].astype(F32)
                first = i * (piece // LANES)
                summed[:, first : first + piece // LANES, :] = total.reshape(
                    chips, piece // LANES, LANES
                ).astype(BF16)
            scatter(summed, results, send2, recv2, peers + [chip], plane)

    for j in (peers + [chip])[::-1]:
        transfer(results.at[j], results.at[j], send2.at[j], recv2.at[j]).wait_recv()

    mixtures = []
    for t in range(count):
        codes = [codes_s[k, t] for k in range(top)]
        mixture = sum(
            results[ids_s[k, t]].astype(F32) * codes[k].astype(F32) for k in range(top)
        )
        mixtures.append(mixture / jnp.full(mixture.shape, sum(codes).astype(F32)))
    mixture = jnp.stack(mixtures).reshape(count, padded)[:, :width]
    out_ref[...] = (tokens_v[...].astype(F32) + mixture).astype(BF16)

    for j in peers:
        transfer(picked.at[j], picked.at[j], send1.at[j], recv1.at[j]).wait_send()
    for j in peers + [chip]:
        transfer(summed.at[j], summed.at[j], send2.at[j], recv2.at[j]).wait_send()
    for g in range(half):
        forward(core, g).wait_send()
    for i in range(pieces):
        exchange(core, i).wait_send()


def shards(tokens, norm_gain, expert_ids, gate_codes, w_gate, w_up, w_down):
    side = math.isqrt(lax.axis_size("ep") // 2)
    chips = side * side
    count, width = tokens.shape
    shard_ff = w_gate.shape[2]
    tiles = 8 * pl.cdiv(width, 8 * LANES)
    pieces = 3
    piece = LANES * (tiles // pieces)
    blocks = pltpu.VMEM((chips, tiles, LANES), BF16)
    turned = pltpu.VMEM((LANES * pl.cdiv(width, LANES), 2 * LANES * pl.cdiv(shard_ff, 2 * LANES)), BF16)
    shares = (pieces, chips, piece)
    DMA = pltpu.SemaphoreType.DMA
    return pl.pallas_call(
        functools.partial(kernel, side, tiles),
        out_shape=jax.ShapeDtypeStruct((count, width), BF16),
        in_specs=[pl.BlockSpec(memory_space=pltpu.HBM)] * 7,
        out_specs=pl.BlockSpec(memory_space=pltpu.VMEM),
        scratch_shapes=[
            pltpu.VMEM((count, width), BF16),
            pltpu.VMEM((width,), F32),
            pltpu.VMEM(expert_ids.shape[::-1], jnp.int32),
            pltpu.SMEM(expert_ids.shape[::-1], jnp.int32),
            pltpu.SMEM(gate_codes.shape[::-1], jnp.int32),
            pltpu.VMEM((shard_ff, width), BF16),
            pltpu.VMEM((shard_ff, width), BF16),
            pltpu.VMEM((shard_ff, width), BF16),
            turned,
            turned,
            blocks,
            pltpu.VMEM((2, chips, tiles, LANES), BF16),
            pltpu.VMEM((chips, tiles * LANES), BF16),
            pltpu.VMEM((2,) + shares, BF16),
            pltpu.VMEM(shares, BF16),
            blocks,
            blocks,
            DMA((5,)),
            DMA((3,)),
            pltpu.SemaphoreType.REGULAR,
            DMA((chips,)),
            DMA((chips,)),
            DMA((side // 2,)),
            DMA((side // 2,)),
            DMA((pieces,)),
            DMA((pieces,)),
            DMA((chips,)),
            DMA((chips,)),
        ],
        compiler_params=pltpu.CompilerParams(
            collective_id=0, has_side_effects=True, vmem_limit_bytes=44 * 2**20
        ),
    )(*[
        pltpu.with_memory_space_constraint(array, pltpu.HBM)
        for array in (
            tokens, norm_gain, expert_ids.T, gate_codes.T,
            jnp.swapaxes(w_gate, 1, 2), jnp.swapaxes(w_up, 1, 2), w_down,
        )
    ])


def solution(mesh):
    return jax.shard_map(
        shards,
        mesh=mesh,
        in_specs=(
            P(("groups", "ep"), None),
            P(),
            P(("groups", "ep"), None),
            P(("groups", "ep"), None),
            P("ep", None, None),
            P("ep", None, None),
            P("ep", None, None),
        ),
        out_specs=P(("groups", "ep"), None),
        check_vma=False,
    )
```

```python
import functools
import math

import jax
import jax.numpy as jnp
from jax import lax
from jax.experimental import pallas as pl
from jax.experimental.pallas import tpu as pltpu
from jax.sharding import PartitionSpec as P

epsilon = 1e-05
MESH = pl.DeviceIdType.MESH
F32 = jnp.float32
BF16 = jnp.bfloat16
LANES = 128


def kernel(
    side, tiles,
    tokens_hbm, gain_hbm, ids_hbm, codes_hbm, gate_hbm, up_hbm, down_hbm,
    out_ref,
    tokens_v, gain_v, ids_v, ids_s, codes_s, gate_v, up_v, down_v, gate_t, up_t,
    picked, slots, arrived, share, taken, summed, results,
    load_sem, weight_sem, ready,
    send1, recv1, send_x, recv_x, send_y, recv_y, send2, recv2,
):
    me = lax.axis_index("ep")
    core = lax.rem(me, 2)
    chip = me // 2
    row, column = chip // side, lax.rem(chip, side)
    chips = side * side
    count, width = tokens_v.shape
    top = ids_v.shape[0]
    padded = tiles * LANES
    partner = {"ep": me + 1 - 2 * core}

    near = lambda d: min(d, side - d)
    offsets = [(dy, dx) for dy in range(side) for dx in range(side) if dy or dx]
    rows_at = [lax.rem(row + d, side) * side for d in range(side)]
    columns_at = [lax.rem(column + d, side) for d in range(side)]
    offsets.sort(key=lambda o: -(near(o[0]) + near(o[1])))
    peers = [rows_at[dy] + columns_at[dx] for dy, dx in offsets]
    offsets.sort(key=lambda o: (-near(o[0]), -near(o[1])))
    peers_back = [rows_at[dy] + columns_at[dx] for dy, dx in offsets]

    barrier = pltpu.get_barrier_semaphore()
    for j in peers:
        pl.semaphore_signal(barrier, inc=1, device_id={"ep": 2 * j + core}, device_id_type=MESH)

    @pl.when(core == 1)
    def _():
        pl.semaphore_signal(barrier, inc=1, device_id=partner, device_id_type=MESH)

    small = [
        pltpu.make_async_copy(src, dst, load_sem.at[i])
        for i, (src, dst) in enumerate(
            [(tokens_hbm, tokens_v), (gain_hbm, gain_v), (ids_hbm, ids_v), (ids_hbm, ids_s), (codes_hbm, codes_s)]
        )
    ]
    for copy in small:
        copy.start()
    weights = [
        pltpu.make_async_copy(src.at[0], dst.at[pl.ds(0, src.shape[1])], weight_sem.at[i])
        for i, (src, dst) in enumerate([(gate_hbm, gate_v), (up_hbm, up_v), (down_hbm, down_v)])
    ]

    for copy in small:
        copy.wait()
    for copy in weights:
        copy.start()

    values = tokens_v[...].astype(F32)
    normed = values * lax.rsqrt(jnp.mean(values * values, axis=1, keepdims=True) + epsilon) * gain_v[...].reshape(1, -1)
    normed = normed.astype(BF16)
    expert = lax.broadcasted_iota(jnp.int32, (chips, count), 0)
    chosen = jnp.zeros(expert.shape, F32)
    for k in range(top):
        chosen = jnp.where(ids_v[k : k + 1, :] == expert, 1.0, chosen)
    rows = jnp.dot(chosen.astype(BF16), normed, preferred_element_type=F32)
    rows = jnp.concatenate([rows, jnp.zeros((chips, padded - width), F32)], axis=1)
    picked[...] = rows.reshape(picked.shape).astype(BF16)
    slots[core, chip] = picked[chip]

    pl.semaphore_wait(barrier, len(peers) + 1 - core)

    @pl.when(core == 0)
    def _():
        pl.semaphore_signal(ready, inc=1, device_id=partner, device_id_type=MESH)

    def scatter(src, dst, send, recv, chips_to, core_to):
        for j in chips_to:
            pltpu.make_async_remote_copy(
                src_ref=src.at[j], dst_ref=dst.at[chip], send_sem=send.at[j], recv_sem=recv.at[chip],
                device_id={"ep": 2 * j + core_to}, device_id_type=MESH,
            ).start()

    def transfer(src, dst, send, recv):
        return pltpu.make_async_remote_copy(
            src_ref=src, dst_ref=dst, send_sem=send, recv_sem=recv, device_id=partner, device_id_type=MESH,
        )

    scatter(picked, slots.at[core], send1, recv1, peers, core)

    arrived[chips:, :] = jnp.zeros((arrived.shape[0] - chips, padded), BF16)
    depth = gate_t.shape[1]
    hidden_size = gate_v.shape[0]
    down_v[hidden_size:, :] = jnp.zeros((depth - hidden_size, width), BF16)
    for i, (src, dst) in enumerate([(gate_v, gate_t), (up_v, up_t)]):
        weights[i].wait()
        dst[:, hidden_size:] = jnp.zeros((dst.shape[0], depth - hidden_size), BF16)
        for low in range(0, width, LANES):
            size = min(LANES, width - low)
            dst[low : low + size, :hidden_size] = src[:, low : low + size].T
        dst[width:, :] = jnp.zeros((dst.shape[0] - width, depth), BF16)

    half = side // 2
    group = 2 * side
    pieces, _, piece = share.shape[1:]
    sizes = [min(piece, width - i * piece) for i in range(pieces)]
    groups = [lax.rem(row // 2 + d, half) for d in sorted(range(half), key=lambda d: min(d, half - d))]

    def forward(plane, g):
        block = slots.at[plane, pl.ds(g * group, group)]
        return transfer(block, block, send_x.at[g], recv_x.at[g])

    def exchange(plane, i):
        return transfer(share.at[plane, i], taken.at[i], send_y.at[i], recv_y.at[i])

    def receive(plane):
        @pl.when(core == plane)
        def _():
            if plane == 1:
                pl.semaphore_wait(ready, 1)
            for n, g in enumerate(groups):
                for i in range(group):
                    j = g * group + i
                    block = slots.at[plane, j]

                    def arrive():
                        transfer(block, block, send1.at[j], recv1.at[j]).wait_recv()

                    if n == 0:
                        pl.when(j != chip)(arrive)
                    else:
                        arrive()
                forward(plane, g).start()

    for plane in (1, 0):
        receive(plane)

        @pl.when(core != plane)
        def _():
            for g in groups:
                forward(plane, g).wait_recv()

        arrived[:chips, :] = slots[plane].reshape(chips, padded)
        rows_in = arrived[:, : gate_t.shape[0]]
        gate_out = jnp.dot(rows_in, gate_t[...], preferred_element_type=F32)
        upward = jnp.dot(rows_in, up_t[...], preferred_element_type=F32)
        hidden = (gate_out / (1.0 + jnp.exp(-gate_out)) * upward).astype(BF16)
        if plane == 1:
            weights[2].wait()
        for i, size in enumerate(sizes):
            low = i * piece
            partial = jnp.dot(
                hidden, down_v[:, low : low + size], preferred_element_type=F32
            ).astype(BF16)
            if size < piece:
                partial = jnp.concatenate([partial, jnp.zeros((partial.shape[0], piece - size), BF16)], axis=1)
            share[plane, i] = partial[:chips]

            @pl.when(core == plane)
            def _():
                exchange(plane, i).start()

        @pl.when(core != plane)
        def _():
            for i in range(pieces):
                exchange(plane, i).wait_recv()
                total = share[plane, i].astype(F32) + taken[i].astype(F32)
                first = i * (piece // LANES)
                summed[:, first : first + piece // LANES, :] = total.reshape(
                    chips, piece // LANES, LANES
                ).astype(BF16)
            scatter(summed, results, send2, recv2, peers_back + [chip], plane)

    for j in (peers_back + [chip])[::-1]:
        transfer(results.at[j], results.at[j], send2.at[j], recv2.at[j]).wait_recv()

    mixtures = []
    for t in range(count):
        codes = [codes_s[k, t] for k in range(top)]
        mixture = sum(
            results[ids_s[k, t]].astype(F32) * codes[k].astype(F32) for k in range(top)
        )
        mixtures.append(mixture / jnp.full(mixture.shape, sum(codes).astype(F32)))
    mixture = jnp.stack(mixtures).reshape(count, padded)[:, :width]
    out_ref[...] = (tokens_v[...].astype(F32) + mixture).astype(BF16)

    for j in peers:
        transfer(picked.at[j], picked.at[j], send1.at[j], recv1.at[j]).wait_send()
    for j in peers + [chip]:
        transfer(summed.at[j], summed.at[j], send2.at[j], recv2.at[j]).wait_send()
    for g in range(half):
        forward(core, g).wait_send()
    for i in range(pieces):
        exchange(core, i).wait_send()


def shards(tokens, norm_gain, expert_ids, gate_codes, w_gate, w_up, w_down):
    side = math.isqrt(lax.axis_size("ep") // 2)
    chips = side * side
    count, width = tokens.shape
    shard_ff = w_gate.shape[2]
    tiles = 8 * pl.cdiv(width, 8 * LANES)
    pieces = 3
    piece = LANES * (tiles // pieces)
    blocks = pltpu.VMEM((chips, tiles, LANES), BF16)
    turned = pltpu.VMEM((LANES * pl.cdiv(width, LANES), 2 * LANES * pl.cdiv(shard_ff, 2 * LANES)), BF16)
    shares = (pieces, chips, piece)
    DMA = pltpu.SemaphoreType.DMA
    return pl.pallas_call(
        functools.partial(kernel, side, tiles),
        out_shape=jax.ShapeDtypeStruct((count, width), BF16),
        in_specs=[pl.BlockSpec(memory_space=pltpu.HBM)] * 7,
        out_specs=pl.BlockSpec(memory_space=pltpu.VMEM),
        scratch_shapes=[
            pltpu.VMEM((count, width), BF16),
            pltpu.VMEM((width,), F32),
            pltpu.VMEM(expert_ids.shape[::-1], jnp.int32),
            pltpu.SMEM(expert_ids.shape[::-1], jnp.int32),
            pltpu.SMEM(gate_codes.shape[::-1], jnp.int32),
            pltpu.VMEM((shard_ff, width), BF16),
            pltpu.VMEM((shard_ff, width), BF16),
            pltpu.VMEM((2 * LANES * pl.cdiv(shard_ff, 2 * LANES), width), BF16),
            turned,
            turned,
            blocks,
            pltpu.VMEM((2, chips, tiles, LANES), BF16),
            pltpu.VMEM((2 * chips, tiles * LANES), BF16),
            pltpu.VMEM((2,) + shares, BF16),
            pltpu.VMEM(shares, BF16),
            blocks,
            blocks,
            DMA((5,)),
            DMA((3,)),
            pltpu.SemaphoreType.REGULAR,
            DMA((chips,)),
            DMA((chips,)),
            DMA((side // 2,)),
            DMA((side // 2,)),
            DMA((pieces,)),
            DMA((pieces,)),
            DMA((chips,)),
            DMA((chips,)),
        ],
        compiler_params=pltpu.CompilerParams(
            collective_id=0, has_side_effects=True, vmem_limit_bytes=44 * 2**20
        ),
    )(*[
        pltpu.with_memory_space_constraint(array, pltpu.HBM)
        for array in (
            tokens, norm_gain, expert_ids.T, gate_codes.T,
            jnp.swapaxes(w_gate, 1, 2), jnp.swapaxes(w_up, 1, 2), w_down,
        )
    ])


def solution(mesh):
    return jax.shard_map(
        shards,
        mesh=mesh,
        in_specs=(
            P(("groups", "ep"), None),
            P(),
            P(("groups", "ep"), None),
            P(("groups", "ep"), None),
            P("ep", None, None),
            P("ep", None, None),
            P("ep", None, None),
        ),
        out_specs=P(("groups", "ep"), None),
        check_vma=False,
    )
```

```python
import functools
import math

import jax
import jax.numpy as jnp
from jax import lax
from jax.experimental import pallas as pl
from jax.experimental.pallas import tpu as pltpu
from jax.sharding import PartitionSpec as P

epsilon = 1e-05
MESH = pl.DeviceIdType.MESH
F32 = jnp.float32
BF16 = jnp.bfloat16
LANES = 128


def kernel(
    side, tiles,
    tokens_hbm, gain_hbm, ids_hbm, codes_hbm, gate_hbm, up_hbm, down_hbm,
    out_ref,
    tokens_v, gain_v, ids_v, ids_s, codes_s, gate_v, up_v, down_v, gate_t, up_t,
    picked, slots, arrived, share, taken, summed, results,
    load_sem, weight_sem, ready,
    send1, recv1, send_x, recv_x, send_y, recv_y, send2, recv2,
):
    me = lax.axis_index("ep")
    core = lax.rem(me, 2)
    chip = me // 2
    row, column = chip // side, lax.rem(chip, side)
    chips = side * side
    count, width = tokens_v.shape
    top = ids_v.shape[0]
    padded = tiles * LANES
    partner = {"ep": me + 1 - 2 * core}

    near = lambda d: min(d, side - d)
    offsets = [(dy, dx) for dy in range(side) for dx in range(side) if dy or dx]
    rows_at = [lax.rem(row + d, side) * side for d in range(side)]
    columns_at = [lax.rem(column + d, side) for d in range(side)]
    offsets.sort(key=lambda o: -(near(o[0]) + near(o[1])))
    peers = [rows_at[dy] + columns_at[dx] for dy, dx in offsets]
    offsets.sort(key=lambda o: (-near(o[0]), -near(o[1])))
    peers_back = [rows_at[dy] + columns_at[dx] for dy, dx in offsets]

    barrier = pltpu.get_barrier_semaphore()
    for j in peers:
        pl.semaphore_signal(barrier, inc=1, device_id={"ep": 2 * j + core}, device_id_type=MESH)

    @pl.when(core == 1)
    def _():
        pl.semaphore_signal(barrier, inc=1, device_id=partner, device_id_type=MESH)

    small = [
        pltpu.make_async_copy(src, dst, load_sem.at[i])
        for i, (src, dst) in enumerate(
            [(tokens_hbm, tokens_v), (gain_hbm, gain_v), (ids_hbm, ids_v), (ids_hbm, ids_s), (codes_hbm, codes_s)]
        )
    ]
    for copy in small:
        copy.start()
    weights = [
        pltpu.make_async_copy(src.at[0], dst.at[pl.ds(0, src.shape[1])], weight_sem.at[i])
        for i, (src, dst) in enumerate([(gate_hbm, gate_v), (up_hbm, up_v), (down_hbm, down_v)])
    ]

    for copy in small:
        copy.wait()
    for copy in weights:
        copy.start()

    values = tokens_v[...].astype(F32)
    normed = values * lax.rsqrt(jnp.mean(values * values, axis=1, keepdims=True) + epsilon) * gain_v[...].reshape(1, -1)
    normed = normed.astype(BF16)
    expert = lax.broadcasted_iota(jnp.int32, (chips, count), 0)
    chosen = jnp.zeros(expert.shape, F32)
    for k in range(top):
        chosen = jnp.where(ids_v[k : k + 1, :] == expert, 1.0, chosen)
    rows = jnp.dot(chosen.astype(BF16), normed, preferred_element_type=F32)
    rows = jnp.concatenate([rows, jnp.zeros((chips, padded - width), F32)], axis=1)
    picked[...] = rows.reshape(picked.shape).astype(BF16)
    slots[core, chip] = picked[chip]

    pl.semaphore_wait(barrier, len(peers) + 1 - core)

    @pl.when(core == 0)
    def _():
        pl.semaphore_signal(ready, inc=1, device_id=partner, device_id_type=MESH)

    def scatter(src, dst, send, recv, chips_to, core_to):
        for j in chips_to:
            pltpu.make_async_remote_copy(
                src_ref=src.at[j], dst_ref=dst.at[chip], send_sem=send.at[j], recv_sem=recv.at[chip],
                device_id={"ep": 2 * j + core_to}, device_id_type=MESH,
            ).start()

    def transfer(src, dst, send, recv):
        return pltpu.make_async_remote_copy(
            src_ref=src, dst_ref=dst, send_sem=send, recv_sem=recv, device_id=partner, device_id_type=MESH,
        )

    scatter(picked, slots.at[core], send1, recv1, peers, core)

    arrived[chips:, :] = jnp.zeros((arrived.shape[0] - chips, padded), BF16)
    depth = gate_t.shape[1]
    hidden_size = gate_v.shape[0]
    down_v[hidden_size:, :] = jnp.zeros((depth - hidden_size, width), BF16)
    for i, (src, dst) in enumerate([(gate_v, gate_t), (up_v, up_t)]):
        weights[i].wait()
        dst[:, hidden_size:] = jnp.zeros((dst.shape[0], depth - hidden_size), BF16)
        for low in range(0, width, LANES):
            size = min(LANES, width - low)
            dst[low : low + size, :hidden_size] = src[:, low : low + size].T
        dst[width:, :] = jnp.zeros((dst.shape[0] - width, depth), BF16)

    half = side // 2
    group = 2 * side
    pieces, _, piece = share.shape[1:]
    sizes = [min(piece, width - i * piece) for i in range(pieces)]
    groups = [lax.rem(row // 2 + d, half) for d in sorted(range(half), key=lambda d: min(d, half - d))]

    def forward(plane, g):
        block = slots.at[plane, pl.ds(g * group, group)]
        return transfer(block, block, send_x.at[g], recv_x.at[g])

    def exchange(plane, i):
        return transfer(share.at[plane, i], taken.at[i], send_y.at[i], recv_y.at[i])

    def receive(plane):
        @pl.when(core == plane)
        def _():
            if plane == 1:
                pl.semaphore_wait(ready, 1)
            for n, g in enumerate(groups):
                for i in range(group):
                    j = g * group + i
                    block = slots.at[plane, j]

                    def arrive():
                        transfer(block, block, send1.at[j], recv1.at[j]).wait_recv()

                    if n == 0:
                        pl.when(j != chip)(arrive)
                    else:
                        arrive()
                forward(plane, g).start()

    early = lax.axis_index("groups") > 0
    pl.when(early)(lambda: receive(0))
    for plane in (1, 0):
        if plane == 1:
            receive(1)
        else:
            pl.when(jnp.logical_not(early))(lambda: receive(0))

        @pl.when(core != plane)
        def _():
            for g in groups:
                forward(plane, g).wait_recv()

        arrived[:chips, :] = slots[plane].reshape(chips, padded)
        rows_in = arrived[:, : gate_t.shape[0]]
        gate_out = jnp.dot(rows_in, gate_t[...], preferred_element_type=F32)
        upward = jnp.dot(rows_in, up_t[...], preferred_element_type=F32)
        hidden = (gate_out / (1.0 + jnp.exp(-gate_out)) * upward).astype(BF16)
        if plane == 1:
            weights[2].wait()
        for i, size in enumerate(sizes):
            low = i * piece
            partial = jnp.dot(
                hidden, down_v[:, low : low + size], preferred_element_type=F32
            ).astype(BF16)
            if size < piece:
                partial = jnp.concatenate([partial, jnp.zeros((partial.shape[0], piece - size), BF16)], axis=1)
            share[plane, i] = partial[:chips]

            @pl.when(core == plane)
            def _():
                exchange(plane, i).start()

        @pl.when(core != plane)
        def _():
            for i in range(pieces):
                exchange(plane, i).wait_recv()
                total = share[plane, i].astype(F32) + taken[i].astype(F32)
                first = i * (piece // LANES)
                summed[:, first : first + piece // LANES, :] = total.reshape(
                    chips, piece // LANES, LANES
                ).astype(BF16)
            scatter(summed, results, send2, recv2, peers_back + [chip], plane)

    for j in peers:
        transfer(picked.at[j], picked.at[j], send1.at[j], recv1.at[j]).wait_send()
    for j in peers + [chip]:
        transfer(summed.at[j], summed.at[j], send2.at[j], recv2.at[j]).wait_send()
    for g in range(half):
        forward(core, g).wait_send()
    for i in range(pieces):
        exchange(core, i).wait_send()

    for j in (peers_back + [chip])[::-1]:
        transfer(results.at[j], results.at[j], send2.at[j], recv2.at[j]).wait_recv()

    mixtures = []
    for t in range(count):
        codes = [codes_s[k, t] for k in range(top)]
        mixture = sum(
            results[ids_s[k, t]].astype(F32) * codes[k].astype(F32) for k in range(top)
        )
        mixtures.append(mixture / jnp.full(mixture.shape, sum(codes).astype(F32)))
    mixture = jnp.stack(mixtures).reshape(count, padded)[:, :width]
    out_ref[...] = (tokens_v[...].astype(F32) + mixture).astype(BF16)


def shards(tokens, norm_gain, expert_ids, gate_codes, w_gate, w_up, w_down):
    side = math.isqrt(lax.axis_size("ep") // 2)
    chips = side * side
    count, width = tokens.shape
    shard_ff = w_gate.shape[2]
    tiles = 8 * pl.cdiv(width, 8 * LANES)
    pieces = 3
    piece = LANES * (tiles // pieces)
    blocks = pltpu.VMEM((chips, tiles, LANES), BF16)
    turned = pltpu.VMEM((LANES * pl.cdiv(width, LANES), 2 * LANES * pl.cdiv(shard_ff, 2 * LANES)), BF16)
    shares = (pieces, chips, piece)
    DMA = pltpu.SemaphoreType.DMA
    return pl.pallas_call(
        functools.partial(kernel, side, tiles),
        out_shape=jax.ShapeDtypeStruct((count, width), BF16),
        in_specs=[pl.BlockSpec(memory_space=pltpu.HBM)] * 7,
        out_specs=pl.BlockSpec(memory_space=pltpu.VMEM),
        scratch_shapes=[
            pltpu.VMEM((count, width), BF16),
            pltpu.VMEM((width,), F32),
            pltpu.VMEM(expert_ids.shape[::-1], jnp.int32),
            pltpu.SMEM(expert_ids.shape[::-1], jnp.int32),
            pltpu.SMEM(gate_codes.shape[::-1], jnp.int32),
            pltpu.VMEM((shard_ff, width), BF16),
            pltpu.VMEM((shard_ff, width), BF16),
            pltpu.VMEM((2 * LANES * pl.cdiv(shard_ff, 2 * LANES), width), BF16),
            turned,
            turned,
            blocks,
            pltpu.VMEM((2, chips, tiles, LANES), BF16),
            pltpu.VMEM((2 * chips, tiles * LANES), BF16),
            pltpu.VMEM((2,) + shares, BF16),
            pltpu.VMEM(shares, BF16),
            blocks,
            blocks,
            DMA((5,)),
            DMA((3,)),
            pltpu.SemaphoreType.REGULAR,
            DMA((chips,)),
            DMA((chips,)),
            DMA((side // 2,)),
            DMA((side // 2,)),
            DMA((pieces,)),
            DMA((pieces,)),
            DMA((chips,)),
            DMA((chips,)),
        ],
        compiler_params=pltpu.CompilerParams(
            collective_id=0, has_side_effects=True, vmem_limit_bytes=44 * 2**20
        ),
    )(*[
        pltpu.with_memory_space_constraint(array, pltpu.HBM)
        for array in (
            tokens, norm_gain, expert_ids.T, gate_codes.T,
            jnp.swapaxes(w_gate, 1, 2), jnp.swapaxes(w_up, 1, 2), w_down,
        )
    ])


def solution(mesh):
    return jax.shard_map(
        shards,
        mesh=mesh,
        in_specs=(
            P(("groups", "ep"), None),
            P(),
            P(("groups", "ep"), None),
            P(("groups", "ep"), None),
            P("ep", None, None),
            P("ep", None, None),
            P("ep", None, None),
        ),
        out_specs=P(("groups", "ep"), None),
        check_vma=False,
    )
```
